32 devices in a mesh: expert: 8 (over z, x), tensor: 4 (over y, core).
Axes of the slice: x: 2, y: 2, z: 4, core: 2. Of those that a mesh axis runs over, the one named last changes fastest.
Arguments:
- hidden_in: bfloat16 [4096, 2048], P('expert', 'tensor'), may hold values from -6 to 6
- out_grad: bfloat16 [4096, 2048], P('expert', 'tensor'), may hold values from -6 to 6
- first_gain: bfloat16 [2048], P('expert'), may hold values from 0.25 to 1.75
- query_weight: bfloat16 [2048, 3072], P('expert', 'tensor'), may hold values from -0.1875 to 0.1875
- latent_weight: bfloat16 [2048, 576], P('expert'), may hold values from -0.125 to 0.125
- latent_gain: bfloat16 [512], P('expert'), may hold values from 0.25 to 1.75
- expand_weight: bfloat16 [512, 4096], P('expert', 'tensor'), may hold values from -0.25 to 0.25
- output_weight: bfloat16 [2048, 2048], P('expert', 'tensor'), may hold values from -0.75 to 0.75
- second_gain: bfloat16 [2048], P('expert'), may hold values from 0.25 to 1.75
- shared_gate: bfloat16 [2048, 2816], P('expert', 'tensor'), may hold values from -0.125 to 0.125
- shared_up: bfloat16 [2048, 2816], P('expert', 'tensor'), may hold values from -0.125 to 0.125
- shared_down: bfloat16 [2048, 2816], P('expert', 'tensor'), may hold values from -0.109375 to 0.109375
- expert_gate: bfloat16 [16, 2048, 1408], P('expert', None, 'tensor'), may hold values from -0.125 to 0.125
- expert_up: bfloat16 [16, 2048, 1408], P('expert', None, 'tensor'), may hold values from -0.125 to 0.125
- expert_down: bfloat16 [16, 1408, 2048], P('expert', 'tensor'), may hold values from -0.15625 to 0.15625
- routes: int32 [4096, 6], P('expert'), may hold values from 0 to 15, all different within a row
- gate_values: float32 [4096, 6], P('expert'), may hold values from 0.3 to 1
Outputs:
- block_out: bfloat16 [4096, 2048], P('expert', 'tensor')
- input_grad: float32 [4096, 2048], P('expert', 'tensor')
- grad_first_gain: float32 [2048], P('expert')
- grad_query: float32 [2048, 3072], P('expert', 'tensor')
- grad_latent: float32 [2048, 576], P('expert')
- grad_latent_gain: float32 [512], P('expert')
- grad_expand: float32 [512, 4096], P('expert', 'tensor')
- grad_output: float32 [2048, 2048], P('expert', 'tensor')
- grad_second_gain: float32 [2048], P('expert')
- grad_shared_gate: float32 [2048, 2816], P('expert', 'tensor')
- grad_shared_up: float32 [2048, 2816], P('expert', 'tensor')
- grad_shared_down: float32 [2048, 2816], P('expert', 'tensor')
- grad_expert_gate: float32 [16, 2048, 1408], P('expert', None, 'tensor')
- grad_expert_up: float32 [16, 2048, 1408], P('expert', None, 'tensor')
- grad_expert_down: float32 [16, 1408, 2048], P('expert', 'tensor')
The draws below stay inside these ranges and needn't reach their ends.
Inputs may be any that keep to these rules, and one draw needn't show every extreme that they name: `routes`: each token names 6 different experts, and every expert is named by some token.
All inputs are finite; a program needn't handle non-finite values.
Results may differ from the reference program's by a relative error of at most 0.025.
Values may be sent and summed in bfloat16 or wider, within the bound.
A program may use at most 320 MiB of HBM per device.

```python
import math
from functools import partial
import jax
import jax.numpy as jnp
from jax import lax

D = 2048
H = 16
DN = 128
DR = 64
DV = 128
KV_RANK = 512
FF = 1408
SH = 2816
TOP = 6
SEQ = 256
BLOCK = 128
EXPERTS = 16
CAP = 128
TOKENS = 4096
N_TENSOR = 4


def shard_levels(stream_key, dims, shards, low, largest):
    loudness = 1.0
    for axis_at, blocks in shards:
        heights = jax.random.uniform(jax.random.fold_in(jax.random.fold_in(stream_key, 6), axis_at), (blocks,), jnp.float32, low / len(shards), largest / len(shards))
        loudness = loudness * jnp.repeat(jnp.exp(heights), dims[axis_at] // blocks).reshape((-1,) + (1,) * (len(dims) - 1 - axis_at))
    return loudness


def picks_of(key, rows, count, top, lift):
    order = jax.random.permutation(jax.random.fold_in(key, 1), count)
    favour = order
    for power in range(3):
        favour = favour * favour // count
    favour = favour * lift // count
    lots = jax.random.randint(jax.random.fold_in(key, 2), (rows, count), 0, 4096) + favour
    sure = jax.random.permutation(jax.random.fold_in(key, 3), rows)[jnp.arange(count) % rows]
    lots = jnp.where(jnp.arange(rows)[:, None] == sure[None, :], 1 << 14, lots)
    score = lots * count + jnp.arange(count)
    return lax.top_k(score.astype(jnp.int32), top)[1].astype(jnp.int32)


def gaussian(key, dims, deviation, most, cuts=(), held_as=jnp.bfloat16):
    drawn = jax.random.normal(key, dims, jnp.float32) * deviation
    if len(cuts) > 0:
        drawn = shard_levels(key, dims, cuts, -0.22, 0.18) * drawn
    return jnp.clip(drawn, min=-most, max=most).astype(held_as)


def setup_inputs(seed: int = 0) -> dict:
    key_of = jax.random.split(jax.random.key(seed), 18)
    return {
        "hidden_in": gaussian(key_of[0], (TOKENS, D), 1.0, 6.0, ((0, 8), (1, 4))),
        "out_grad": gaussian(key_of[1], (TOKENS, D), 1.0, 6.0, ((0, 8), (1, 4))),
        "first_gain": jnp.clip(1.0 + 0.15 * jax.random.normal(key_of[2], (D,), jnp.float32), 0.25, 1.75).astype(jnp.bfloat16),
        "query_weight": gaussian(key_of[3], (D, H * (DN + DR)), (D // 2) ** -0.5, 0.1875, ((0, 8), (1, 4))),
        "latent_weight": gaussian(key_of[4], (D, KV_RANK + DR), D ** -0.5, 0.125, ((0, 8),)),
        "latent_gain": jnp.clip(1.0 + 0.15 * jax.random.normal(key_of[5], (KV_RANK,), jnp.float32), 0.25, 1.75).astype(jnp.bfloat16),
        "expand_weight": gaussian(key_of[6], (KV_RANK, H * (DN + DV)), KV_RANK ** -0.5, 0.25, ((0, 8), (1, 4))),
        "output_weight": gaussian(key_of[7], (D, H * DV), (H * DV // 32) ** -0.5, 0.75, ((0, 8), (1, 4))),
        "second_gain": jnp.clip(1.0 + 0.15 * jax.random.normal(key_of[8], (D,), jnp.float32), 0.25, 1.75).astype(jnp.bfloat16),
        "shared_gate": gaussian(key_of[9], (D, SH), D ** -0.5, 0.125, ((0, 8), (1, 4))),
        "shared_up": gaussian(key_of[10], (D, SH), D ** -0.5, 0.125, ((0, 8), (1, 4))),
        "shared_down": gaussian(key_of[11], (D, SH), SH ** -0.5, 0.109375, ((0, 8), (1, 4))),
        "expert_gate": gaussian(key_of[12], (EXPERTS, D, FF), D ** -0.5, 0.125, ((0, 8), (2, 4))),
        "expert_up": gaussian(key_of[13], (EXPERTS, D, FF), D ** -0.5, 0.125, ((0, 8), (2, 4))),
        "expert_down": gaussian(key_of[14], (EXPERTS, FF, D), FF ** -0.5, 0.15625, ((0, 8), (1, 4))),
        "routes": picks_of(key_of[15], TOKENS, EXPERTS, TOP, 3072),
        "gate_values": jnp.clip(0.3 + 0.7 * jax.random.uniform(key_of[16], (TOKENS, TOP), jnp.float32) ** shard_levels(key_of[16], (TOKENS, TOP), ((0, 8),), -0.2, 0.2), 0.3, 1.0),
    }


@jax.custom_vjp
def low(v):
    return lax.optimization_barrier(v.astype(jnp.bfloat16)).astype(jnp.float32)

@jax.custom_vjp
def low_back(v):
    return v

def low_keep(v):
    return (low(v), None)

def low_pass(kept, grad):
    return (grad,)

def back_keep(v):
    return (v, None)

def back_low(kept, grad):
    return (low(grad),)
low.defvjp(low_keep, low_pass)
low_back.defvjp(back_keep, back_low)
precise = lax.Precision.HIGHEST
norm_eps = 1e-06
masked_value = -1000000000.0

def matmul(left, right):
    return jnp.dot(left, right, precision=precise, preferred_element_type=jnp.float32)

def rms_scale(values):
    return lax.rsqrt(lax.optimization_barrier(jnp.mean(values * values, axis=-1, keepdims=True)) + norm_eps)

def rope_tables(length, width):
    position = jnp.arange(length, dtype=jnp.float32)
    rates = jnp.exp(jnp.arange(width // 2, dtype=jnp.float32) * (-2.0 * math.log(10000.0) / width))
    angle = position[:, None] * rates[None, :]
    return (jnp.cos(angle), jnp.sin(angle))

def rotate(values, cosine, sine):
    half = values.shape[-1] // 2
    first = values[..., :half]
    second = values[..., half:]
    return jnp.concatenate([first * cosine - second * sine, second * cosine + first * sine], axis=-1)

def slot_targets(route_rows, experts_all, capacity):
    length = route_rows.shape[0]
    onehot = (route_rows[:, :, None] == jnp.arange(experts_all, dtype=jnp.int32)[None, None, :]).astype(jnp.int32)
    per_token = lax.optimization_barrier(jnp.sum(onehot, axis=1)).astype(jnp.int32)
    prior = (jnp.cumsum(per_token, axis=0).astype(jnp.int32) - per_token).astype(jnp.int32)
    rank = jnp.take_along_axis(prior, route_rows, axis=1).astype(jnp.int32)
    kept = rank < capacity
    targets = jnp.where(kept, route_rows * capacity + rank, experts_all * capacity).astype(jnp.int32)
    owners = jnp.full((experts_all * capacity,), length, jnp.int32).at[targets.reshape(-1)].set(jnp.repeat(jnp.arange(length, dtype=jnp.int32), route_rows.shape[1]), mode='drop')
    return (targets, owners)

def pick_rows(table, index):
    return table[index]

def expert_apply(item):
    rows, gate_w, up_w, down_w = item
    quarter = FF // N_TENSOR
    total = jnp.zeros(rows.shape, jnp.float32)
    for part in range(N_TENSOR):
        lower = part * quarter
        inputs = low_back(rows)
        gated = low_back(matmul(inputs, gate_w[:, lower:lower + quarter]))
        upper = low_back(matmul(inputs, up_w[:, lower:lower + quarter]))
        hidden = low(jax.nn.silu(gated) * upper)
        total = total + low(matmul(hidden, down_w[lower:lower + quarter, :]))
    return low_back(total)

def forward(hidden_in, first_gain, query_weight, latent_weight, latent_gain, expand_weight, output_weight, second_gain, shared_gate, shared_up, shared_down, expert_gate, expert_up, expert_down, targets, owners, gate_values):
    count = hidden_in.shape[0] // SEQ
    cosine, sine = rope_tables(SEQ, DR)
    blocks = jnp.arange(SEQ, dtype=jnp.int32) // BLOCK
    allowed = blocks[None, :] <= blocks[:, None]
    normed = low(hidden_in * rms_scale(hidden_in) * first_gain)
    query = low_back(matmul(normed, query_weight)).reshape(count, SEQ, H, DN + DR)
    latent = low_back(matmul(normed, latent_weight)).reshape(count, SEQ, KV_RANK + DR)
    compressed = latent[..., :KV_RANK]
    latent_normed = low(compressed * rms_scale(compressed) * latent_gain)
    expanded = low_back(matmul(latent_normed.reshape(-1, KV_RANK), expand_weight)).reshape(count, SEQ, H, DN + DV)
    queries = low(jnp.concatenate([query[..., :DN], rotate(query[..., DN:], cosine[:, None, :], sine[:, None, :])], axis=-1))
    key_rope = rotate(latent[..., KV_RANK:], cosine, sine)
    keys = low(jnp.concatenate([expanded[..., :DN], jnp.broadcast_to(key_rope[:, :, None, :], (count, SEQ, H, DR))], axis=-1))
    values = low(expanded[..., DN:])
    scores = low_back(jnp.einsum('nqhc,nkhc->nhqk', queries, keys, precision=precise) * (DN + DR) ** (-0.5))
    masked = jnp.where(allowed, scores, masked_value)
    softmax_weights = jnp.exp(masked - jax.nn.logsumexp(masked, axis=-1, keepdims=True))
    mixed = low_back(low(jnp.einsum('nhqk,nkhc->nqhc', low(softmax_weights), values, precision=precise)))
    attended = low_back(matmul(mixed.reshape(-1, H * DV), output_weight.T))
    middle = hidden_in + attended
    mixer_in = low(middle * rms_scale(middle) * second_gain)
    shared_g = low_back(matmul(mixer_in, shared_gate))
    shared_u = low_back(matmul(mixer_in, shared_up))
    shared_out = matmul(low(jax.nn.silu(shared_g) * shared_u), shared_down.T)
    padded_in = jnp.concatenate([mixer_in.reshape(count, SEQ, D), jnp.zeros((count, 1, D), jnp.float32)], axis=1)
    dispatched = jax.vmap(pick_rows)(padded_in, owners)
    stacked = jnp.moveaxis(dispatched.reshape(count, EXPERTS, CAP, D), 1, 0).reshape(EXPERTS, count * CAP, D)
    outputs = lax.map(jax.checkpoint(expert_apply), (stacked, expert_gate, expert_up, expert_down))
    returned = jnp.moveaxis(outputs.reshape(EXPERTS, count, CAP, D), 0, 1).reshape(count, EXPERTS * CAP, D)
    padded_out = jnp.concatenate([returned, jnp.zeros((count, 1, D), jnp.float32)], axis=1)
    picked = jax.vmap(pick_rows)(padded_out, targets.reshape(count, SEQ * TOP)).reshape(count * SEQ, TOP, D)
    routed = lax.optimization_barrier(jnp.sum(gate_values[:, :, None] * picked, axis=1))
    return middle + shared_out + routed

def reference(hidden_in, out_grad, first_gain, query_weight, latent_weight, latent_gain, expand_weight, output_weight, second_gain, shared_gate, shared_up, shared_down, expert_gate, expert_up, expert_down, routes, gate_values):
    count = routes.shape[0] // SEQ
    targets, owners = jax.vmap(partial(slot_targets, experts_all=EXPERTS, capacity=CAP))(routes.reshape(count, SEQ, TOP))
    floats = tuple((item.astype(jnp.float32) for item in (hidden_in, first_gain, query_weight, latent_weight, latent_gain, expand_weight, output_weight, second_gain, shared_gate, shared_up, shared_down, expert_gate, expert_up, expert_down)))
    gates_f = gate_values.astype(jnp.float32)

    def closed(*params):
        return forward(*params, targets, owners, gates_f)
    result, pullback = jax.vjp(closed, *floats)
    grads = pullback(out_grad.astype(jnp.float32))
    return (result.astype(jnp.bfloat16), grads[0], grads[1], grads[2], grads[3], grads[4], grads[5], grads[6], grads[7], grads[8], grads[9], grads[10], grads[11], grads[12], grads[13])
```

```python
import functools
import math

import jax
import jax.numpy as jnp
from jax import lax
from jax.experimental import pallas as pl
from jax.experimental.pallas import tpu as pltpu
from jax.sharding import PartitionSpec as P

D = 2048
H = 16
DN = 128
DR = 64
DV = 128
KV_RANK = 512
TOP = 6
EXP_DEV = 2
SEQ = 256
BLOCK = 128

norm_eps = 1e-06
masked_value = -1000000000.0
BF = jnp.bfloat16
F32 = jnp.float32


def matmul(left, right):
    return jnp.dot(left, right, preferred_element_type=F32)


def matmul_rows(left, right):
    return lax.dot_general(left, right, (((1,), (1,)), ((), ())), preferred_element_type=F32)


def matmul_cols(left, right):
    return lax.dot_general(left, right, (((0,), (0,)), ((), ())), preferred_element_type=F32)


def rms_scale(values):
    return lax.rsqrt(jnp.mean(values * values, axis=-1, keepdims=True) + norm_eps)


def rope_tables(length, width):
    position = jnp.arange(length, dtype=F32)
    rates = jnp.exp(jnp.arange(width // 2, dtype=F32) * (-2.0 * math.log(10000.0) / width))
    angle = position[:, None] * rates[None, :]
    return (jnp.cos(angle), jnp.sin(angle))


def rotate(values, cosine, sine):
    half = values.shape[-1] // 2
    first = values[..., :half]
    second = values[..., half:]
    return jnp.concatenate(
        [first * cosine - second * sine, second * cosine + first * sine], axis=-1
    )


def unrotate(grads, cosine, sine):
    half = grads.shape[-1] // 2
    first = grads[..., :half]
    second = grads[..., half:]
    return jnp.concatenate(
        [first * cosine + second * sine, second * cosine - first * sine], axis=-1
    )


def norm_back(grad_hat, hat, scale_rows):
    return scale_rows * (grad_hat - hat * jnp.mean(grad_hat * hat, axis=-1, keepdims=True))


def expert_kernel(
    seqs, cap, tensors, slots, gates, x, og, wgu, wd, out, dgu, dd, xs, gs, parts, backs, acc_gu, acc_d, sems
):
    step = pl.program_id(0)
    width = x.shape[-1]
    half = wd.shape[1]

    @pl.when(step == 0)
    def _():
        acc_gu[...] = jnp.zeros_like(acc_gu)
        acc_d[...] = jnp.zeros_like(acc_d)

    iota = lax.broadcasted_iota(jnp.int32, (cap, SEQ), 0)
    picks = []
    slot_gates = []
    for s in range(seqs):
        chosen = []
        for e in range(EXP_DEV):
            row = s * EXP_DEV + e
            hit = iota == slots[0, row : row + 1, :]
            slot_gates.append(
                jnp.sum(jnp.where(hit, gates[0, row : row + 1, :], 0.0), axis=1, keepdims=True)
            )
            chosen.append(hit.astype(F32).astype(BF))
        picks.append(jnp.concatenate(chosen, axis=0))
    for s in range(seqs):
        for t in range(tensors):
            cols = slice(t * width, (t + 1) * width)
            rows = slice(s * SEQ, (s + 1) * SEQ)
            got = matmul(picks[s], x[0, t, rows, :])
            grad = matmul(picks[s], og[0, t, rows, :])
            for e in range(EXP_DEV):
                xs[e, s * cap : (s + 1) * cap, cols] = got[e * cap : (e + 1) * cap].astype(BF)
                gs[e, s * cap : (s + 1) * cap, cols] = (
                    grad[e * cap : (e + 1) * cap] * slot_gates[s * EXP_DEV + e]
                ).astype(BF)
    for e in range(EXP_DEV):
        gate_col = jnp.concatenate([slot_gates[s * EXP_DEV + e] for s in range(seqs)], axis=0)
        both = matmul(xs[e], wgu[e])
        gated = both[:, :half]
        upper = both[:, half:]
        sig = jax.nn.sigmoid(gated)
        act = gated * sig
        hidden = (act * upper).astype(BF)
        grad_hidden = matmul_rows(gs[e], wd[e])
        grad_gu = jnp.concatenate(
            [
                (grad_hidden * upper * sig * (1.0 + gated * (1.0 - sig))).astype(BF),
                (grad_hidden * act).astype(BF),
            ],
            axis=1,
        )
        part = (matmul(hidden, wd[e]) * gate_col).astype(BF)
        back = matmul_rows(grad_gu, wgu[e]).astype(BF)
        for s in range(seqs):
            parts[s, e * cap : (e + 1) * cap, :] = part[s * cap : (s + 1) * cap]
            backs[s, e * cap : (e + 1) * cap, :] = back[s * cap : (s + 1) * cap]
        acc_d[e] += matmul_cols(hidden, gs[e])
        acc_gu[e] += matmul_cols(xs[e], grad_gu)
    for s in range(seqs):
        for t in range(tensors):
            cols = slice(t * width, (t + 1) * width)
            rows = slice(s * SEQ, (s + 1) * SEQ)
            out[0, t, 0, rows, :] = matmul_cols(picks[s], parts[s, :, cols]).astype(BF)
            out[0, t, 1, rows, :] = matmul_cols(picks[s], backs[s, :, cols]).astype(BF)

    @pl.when(step == pl.num_programs(0) - 1)
    def _():
        first = pltpu.make_async_copy(acc_gu, dgu, sems.at[0])
        second = pltpu.make_async_copy(acc_d, dd, sems.at[1])
        first.start()
        second.start()
        first.wait()
        second.wait()


def run_experts(slots, gates, x, og, wgu, wd, cap):
    groups, tensors, count, width = x.shape
    seqs = count // SEQ
    half = wd.shape[1]
    rows = slots.shape[1]
    stream = lambda g: (g, 0, 0, 0)
    return pl.pallas_call(
        functools.partial(expert_kernel, seqs, cap, tensors),
        grid=(groups,),
        in_specs=[
            pl.BlockSpec((1, rows, SEQ), lambda g: (g, 0, 0)),
            pl.BlockSpec((1, rows, SEQ), lambda g: (g, 0, 0)),
            pl.BlockSpec((1, tensors, count, width), stream),
            pl.BlockSpec((1, tensors, count, width), stream),
            pl.BlockSpec(wgu.shape, lambda g: (0, 0, 0), pipeline_mode=pl.Buffered(1)),
            pl.BlockSpec(wd.shape, lambda g: (0, 0, 0), pipeline_mode=pl.Buffered(1)),
        ],
        out_specs=[
            pl.BlockSpec((1, tensors, 2, count, width), lambda g: (g, 0, 0, 0, 0)),
            pl.BlockSpec(memory_space=pl.ANY),
            pl.BlockSpec(memory_space=pl.ANY),
        ],
        out_shape=[
            jax.ShapeDtypeStruct((groups, tensors, 2, count, width), BF),
            jax.ShapeDtypeStruct(wgu.shape, F32),
            jax.ShapeDtypeStruct(wd.shape, F32),
        ],
        scratch_shapes=[
            pltpu.VMEM((EXP_DEV, seqs * cap, D), BF),
            pltpu.VMEM((EXP_DEV, seqs * cap, D), BF),
            pltpu.VMEM((seqs, EXP_DEV * cap, D), BF),
            pltpu.VMEM((seqs, EXP_DEV * cap, D), BF),
            pltpu.VMEM(wgu.shape, F32),
            pltpu.VMEM(wd.shape, F32),
            pltpu.SemaphoreType.DMA((2,)),
        ],
        compiler_params=pltpu.CompilerParams(
            dimension_semantics=("arbitrary",), vmem_limit_bytes=60 * 1024 * 1024
        ),
        cost_estimate=pl.CostEstimate(
            flops=groups * EXP_DEV * seqs * cap * D * (half * 18 + SEQ * 8),
            bytes_accessed=groups * tensors * count * width * 8 + wgu.size * 9,
            transcendentals=groups * EXP_DEV * seqs * cap * half,
        ),
        name="experts",
    )(slots, gates, x, og, wgu, wd)


def local(
    hidden_in,
    out_grad,
    first_gain,
    query_weight,
    latent_weight,
    latent_gain,
    expand_weight,
    output_weight,
    second_gain,
    shared_gate,
    shared_up,
    shared_down,
    expert_gate,
    expert_up,
    expert_down,
    routes,
    gate_values,
):
    groups = lax.axis_size("expert")
    tensors = lax.axis_size("tensor")
    place = lax.axis_index("tensor")
    mine = lax.axis_index("expert")
    experts_all = EXP_DEV * groups
    cap = SEQ * TOP * 4 // (3 * experts_all)
    width = D // tensors
    heads = H // tensors
    count = hidden_in.shape[0]
    seqs = count // SEQ
    rows_dev = D // groups
    scale = (DN + DR) ** (-0.5)
    cosine, sine = rope_tables(SEQ, DR)
    blocks = jnp.arange(SEQ, dtype=jnp.int32) // BLOCK
    allowed = (blocks[None, :] <= blocks[:, None])[None, None]

    whole_in = lax.all_gather(hidden_in, "tensor", axis=1, tiled=True)
    qc = query_weight.shape[1]
    oc = output_weight.shape[1]
    lc = latent_weight.shape[1]
    sc = shared_gate.shape[1]
    er, ec = expand_weight.shape
    cut = er * ec // rows_dev
    fold = rows_dev // er
    expand_rows = jnp.concatenate(
        [expand_weight[:, i * cut : (i + 1) * cut] for i in range(fold)], axis=0
    )
    attn_all = lax.all_gather(
        jnp.concatenate([query_weight, output_weight, expand_rows, latent_weight], axis=1),
        "expert",
        axis=0,
        tiled=True,
    )
    full_query = attn_all[:, :qc]
    full_output = attn_all[:, qc : qc + oc]
    full_latent = attn_all[:, qc + oc + cut :]
    full_expand = (
        attn_all[:, qc + oc : qc + oc + cut]
        .reshape(groups, fold, er, cut)
        .transpose(0, 2, 1, 3)
        .reshape(groups * er, ec)
    )
    gains = lax.all_gather(
        jnp.concatenate([first_gain, second_gain, latent_gain]).astype(F32), "expert", axis=0
    )
    gain_first = gains[:, :rows_dev].reshape(-1)
    gain_mid = gains[:, rows_dev : 2 * rows_dev].reshape(-1)
    gain_kv = gains[:, 2 * rows_dev :].reshape(-1)
    table = lax.all_gather(
        jnp.concatenate([routes.T.astype(F32), gate_values.T], axis=0), "expert", axis=0
    )
    pieces = max(1, min(seqs, groups // 8))
    per = count // pieces

    def to_all(rows):
        return lax.all_gather(rows, ("expert", "tensor"), axis=0).reshape(
            groups, tensors, per, width
        )

    og_first = to_all(out_grad[:per])
    shared_all = lax.all_gather(
        jnp.concatenate([shared_gate, shared_up, shared_down], axis=1), "expert", axis=0, tiled=True
    )
    full_sgu = shared_all[:, : 2 * sc]
    full_sdown = shared_all[:, 2 * sc :]

    inputs = whole_in.astype(F32)
    first_scale = rms_scale(inputs)
    first_hat = inputs * first_scale
    normed = (first_hat * gain_first).astype(BF)
    query = matmul(normed, full_query).reshape(seqs, SEQ, heads, DN + DR)
    latent = matmul(normed, full_latent)
    compressed = latent[:, :KV_RANK]
    latent_scale = rms_scale(compressed)
    latent_hat = compressed * latent_scale
    latent_normed = (latent_hat * gain_kv).astype(BF)
    expanded = matmul(latent_normed, full_expand).reshape(seqs, SEQ, heads, DN + DV)
    queries = jnp.concatenate(
        [query[..., :DN], rotate(query[..., DN:], cosine[:, None, :], sine[:, None, :])], axis=-1
    ).astype(BF)
    key_rope = rotate(latent[:, KV_RANK:].reshape(seqs, SEQ, DR), cosine, sine).astype(BF)
    keys = jnp.concatenate(
        [
            expanded[..., :DN].astype(BF),
            jnp.broadcast_to(key_rope[:, :, None, :], (seqs, SEQ, heads, DR)),
        ],
        axis=-1,
    )
    values = expanded[..., DN:].astype(BF)
    scores = jnp.where(
        allowed,
        jnp.einsum("nqhc,nkhc->nhqk", queries, keys, preferred_element_type=F32) * scale,
        masked_value,
    )
    peak = jnp.max(scores, axis=-1, keepdims=True)
    log_total = peak + jnp.log(jnp.sum(jnp.exp(scores - peak), axis=-1, keepdims=True))
    weights = jnp.exp(scores - log_total)
    mixed = (
        jnp.einsum("nhqk,nkhc->nqhc", weights.astype(BF), values, preferred_element_type=F32)
        .astype(BF)
        .reshape(count, heads * DV)
    )
    attended = lax.psum(matmul_rows(mixed, full_output).astype(BF), "tensor").astype(F32)
    middle = inputs + attended
    second_scale = rms_scale(middle)
    second_hat = middle * second_scale
    mixer_in = (second_hat * gain_mid).astype(BF)
    mixer_slice = lax.dynamic_slice_in_dim(mixer_in, place * width, width, 1)

    local_experts = (mine * EXP_DEV + jnp.arange(EXP_DEV, dtype=jnp.int32)).astype(F32)
    route_t = table[:, :TOP].reshape(groups, TOP, seqs, SEQ)
    gate_t = table[:, TOP:].reshape(groups, TOP, seqs, SEQ)
    named = route_t[:, :, :, None, :] == local_experts[None, None, None, :, None]
    gate_of = jnp.sum(jnp.where(named, gate_t[:, :, :, None, :], 0.0), axis=1)
    used = jnp.any(named, axis=1)
    before = (
        jnp.arange(SEQ, dtype=jnp.int32)[:, None] < jnp.arange(SEQ, dtype=jnp.int32)[None, :]
    ).astype(BF)
    prior = jnp.einsum("gset,tu->gseu", used.astype(BF), before, preferred_element_type=F32)
    slot_of = jnp.where(used & (prior < cap), prior, -1.0).astype(jnp.int32)
    slot_of = slot_of.reshape(groups, seqs * EXP_DEV, SEQ)
    gate_of = gate_of.reshape(groups, seqs * EXP_DEV, SEQ)

    ff = expert_gate.shape[2]
    half = -(-ff // 128) * 128
    wide = ((0, 0), (0, 0), (0, half - ff))
    wgu = jnp.concatenate([jnp.pad(expert_gate, wide), jnp.pad(expert_up, wide)], axis=2)
    wd = jnp.pad(expert_down, ((0, 0), (0, half - ff), (0, 0)))
    rows = slot_of.shape[1] // pieces
    sums = []
    dgu = dd = None
    for i in range(pieces):
        span = slice(i * per, (i + 1) * per)
        mixer_rows, og_rows = mixer_slice[span], out_grad[span]
        if i > 0:
            mixer_rows, og_rows, *sums = lax.optimization_barrier((mixer_rows, og_rows, *sums))
        outs, g_gu, g_d = run_experts(
            slot_of[:, i * rows : (i + 1) * rows],
            gate_of[:, i * rows : (i + 1) * rows],
            to_all(mixer_rows),
            og_first if i == 0 else to_all(og_rows),
            wgu,
            wd,
            cap,
        )
        dgu = g_gu if dgu is None else dgu + g_gu
        dd = g_d if dd is None else dd + g_d
        summed = lax.psum_scatter(
            outs.reshape(groups * tensors * 2 * per, width),
            ("expert", "tensor"),
            scatter_dimension=0,
            tiled=True,
        )
        sums.append(summed.reshape(2, per, width))
    summed = jnp.concatenate(sums, axis=1) if pieces > 1 else sums[0]
    total_gate = dgu[:, :, :ff]
    total_up = dgu[:, :, half : half + ff]
    total_down = dd[:, :ff]

    if pieces == 1:
        whole_grad = lax.dynamic_slice_in_dim(og_first, mine, 1, 0)[0]
        whole_grad = whole_grad.transpose(1, 0, 2).reshape(count, D)
    else:
        whole_grad = lax.all_gather(out_grad, "tensor", axis=1, tiled=True)
    shared_gu = matmul(mixer_in, full_sgu)
    shared_g = shared_gu[:, :sc]
    shared_u = shared_gu[:, sc:]
    shared_sig = jax.nn.sigmoid(shared_g)
    shared_hidden = (shared_g * shared_sig * shared_u).astype(BF)
    shared_part = matmul_rows(shared_hidden, full_sdown)
    grad_shared = matmul(whole_grad, full_sdown)
    step_sdown = matmul_cols(whole_grad, shared_hidden)
    grad_sg = (grad_shared * shared_u * shared_sig * (1.0 + shared_g * (1.0 - shared_sig))).astype(
        BF
    )
    grad_su = (grad_shared * shared_g * shared_sig).astype(BF)
    grad_sgu = jnp.concatenate([grad_sg, grad_su], axis=1)
    step_sgu = matmul_cols(mixer_in, grad_sgu)
    mixer_part = matmul_rows(grad_sgu, full_sgu)
    shared_sums = lax.psum_scatter(
        jnp.concatenate([shared_part.astype(BF), mixer_part.astype(BF)], axis=0),
        "tensor",
        scatter_dimension=1,
        tiled=True,
    )
    middle_slice = lax.dynamic_slice_in_dim(middle, place * width, width, 1)
    block_out = (
        middle_slice + summed[0].astype(F32) + shared_sums[:count].astype(F32)
    ).astype(BF)
    grad_mixer = lax.all_gather(
        (summed[1].astype(F32) + shared_sums[count:].astype(F32)).astype(BF),
        "tensor",
        axis=1,
        tiled=True,
    ).astype(F32)
    shared_steps = lax.psum_scatter(
        jnp.concatenate([step_sgu.astype(BF), step_sdown.astype(BF)], axis=1),
        "expert",
        scatter_dimension=0,
        tiled=True,
    ).astype(F32)

    step_gain_two = jnp.sum(grad_mixer * second_hat, axis=0)
    grad_middle = whole_grad.astype(F32) + norm_back(
        grad_mixer * gain_mid, second_hat, second_scale
    )
    grad_att = grad_middle.astype(BF)
    step_output = matmul_cols(grad_att, mixed)
    grad_mixed = matmul(grad_att, full_output).astype(BF).reshape(seqs, SEQ, heads, DV)
    grad_weights = jnp.einsum(
        "nqhc,nkhc->nhqk", grad_mixed, values, preferred_element_type=F32
    )
    grad_scores = (
        weights * (grad_weights - jnp.sum(weights * grad_weights, axis=-1, keepdims=True))
    ).astype(BF)
    grad_values = jnp.einsum(
        "nhqk,nqhc->nkhc", weights.astype(BF), grad_mixed, preferred_element_type=F32
    )
    grad_queries = (
        jnp.einsum("nhqk,nkhc->nqhc", grad_scores, keys, preferred_element_type=F32) * scale
    )
    grad_keys = (
        jnp.einsum("nhqk,nqhc->nkhc", grad_scores, queries, preferred_element_type=F32) * scale
    )
    grad_query = (
        jnp.concatenate(
            [
                grad_queries[..., :DN],
                unrotate(grad_queries[..., DN:], cosine[:, None, :], sine[:, None, :]),
            ],
            axis=-1,
        )
        .astype(BF)
        .reshape(count, heads * (DN + DR))
    )
    step_query = matmul_cols(normed, grad_query)
    query_part = matmul_rows(grad_query, full_query)
    rope_part = unrotate(jnp.sum(grad_keys[..., DN:], axis=2), cosine, sine).reshape(count, DR)
    grad_expanded = (
        jnp.concatenate([grad_keys[..., :DN], grad_values], axis=-1)
        .astype(BF)
        .reshape(count, heads * (DN + DV))
    )
    step_expand = matmul_cols(latent_normed, grad_expanded)
    latent_part = matmul_rows(grad_expanded, full_expand)
    latent_sum = lax.psum(
        jnp.concatenate([latent_part.astype(BF), rope_part.astype(BF)], axis=1), "tensor"
    ).astype(F32)
    grad_lnormed = latent_sum[:, :KV_RANK]
    step_gain_latent = jnp.sum(grad_lnormed * latent_hat, axis=0)
    grad_compressed = norm_back(grad_lnormed * gain_kv, latent_hat, latent_scale)
    grad_lat = jnp.concatenate([grad_compressed, latent_sum[:, KV_RANK:]], axis=-1).astype(BF)
    step_latent = matmul_cols(normed, grad_lat)
    query_sum = lax.psum_scatter(
        query_part.astype(BF), "tensor", scatter_dimension=1, tiled=True
    ).astype(F32)
    latent_slice = lax.dynamic_slice_in_dim(full_latent, place * width, width, 0)
    grad_normed = query_sum + matmul_rows(grad_lat, latent_slice)
    first_hat_slice = lax.dynamic_slice_in_dim(first_hat, place * width, width, 1)
    gain_first_slice = lax.dynamic_slice_in_dim(gain_first, place * width, width, 0)
    grad_hat = grad_normed * gain_first_slice
    row_dot = lax.psum(jnp.sum(grad_hat * first_hat_slice, axis=1), "tensor") / D
    grad_middle_slice = lax.dynamic_slice_in_dim(grad_middle, place * width, width, 1)
    input_grad = grad_middle_slice + first_scale * (grad_hat - first_hat_slice * row_dot[:, None])
    step_gain_one = jnp.sum(grad_normed * first_hat_slice, axis=0)

    expand_back = (
        step_expand.astype(BF)
        .reshape(groups, er, fold, cut)
        .transpose(0, 2, 1, 3)
        .reshape(groups * rows_dev, cut)
    )
    attn_steps = lax.psum_scatter(
        jnp.concatenate(
            [step_query.astype(BF), step_output.astype(BF), expand_back, step_latent.astype(BF)],
            axis=1,
        ),
        "expert",
        scatter_dimension=0,
        tiled=True,
    ).astype(F32)
    grad_expand = attn_steps[:, qc + oc : qc + oc + cut]
    grad_expand = jnp.concatenate(
        [grad_expand[i * er : (i + 1) * er] for i in range(fold)], axis=1
    )
    one_full = lax.dynamic_update_slice_in_dim(
        jnp.zeros((D,), F32), step_gain_one, place * width, 0
    )
    gain_sums = lax.psum(
        jnp.concatenate([one_full, step_gain_two / tensors, step_gain_latent / tensors]),
        ("expert", "tensor"),
    )
    kv_dev = latent_gain.shape[0]
    return (
        block_out,
        input_grad,
        lax.dynamic_slice_in_dim(gain_sums, mine * rows_dev, rows_dev, 0),
        attn_steps[:, :qc],
        attn_steps[:, qc + oc + cut :],
        lax.dynamic_slice_in_dim(gain_sums, 2 * D + mine * kv_dev, kv_dev, 0),
        grad_expand,
        attn_steps[:, qc : qc + oc],
        lax.dynamic_slice_in_dim(gain_sums, D + mine * rows_dev, rows_dev, 0),
        shared_steps[:, :sc],
        shared_steps[:, sc : 2 * sc],
        shared_steps[:, 2 * sc :],
        total_gate,
        total_up,
        total_down,
    )


def solution(mesh):
    both = P("expert", "tensor")
    cols = P("expert", None, "tensor")
    rows = P("expert", "tensor", None)
    one = P("expert")
    flat = P("expert", None)
    return jax.shard_map(
        local,
        mesh=mesh,
        in_specs=(
            both, both, one, both, flat, one, both, both, one, both, both, both,
            cols, cols, rows, flat, flat,
        ),
        out_specs=(
            both, both, one, both, flat, one, both, both, one, both, both, both,
            cols, cols, rows,
        ),
        check_vma=False,
    )
```

```python
import functools
import math

import jax
import jax.numpy as jnp
from jax import lax
from jax.experimental import pallas as pl
from jax.experimental.pallas import tpu as pltpu
from jax.sharding import PartitionSpec as P

D = 2048
H = 16
DN = 128
DR = 64
DV = 128
KV_RANK = 512
TOP = 6
EXP_DEV = 2
SEQ = 256
BLOCK = 128

norm_eps = 1e-06
masked_value = -1000000000.0
BF = jnp.bfloat16
F32 = jnp.float32


def matmul(left, right):
    return jnp.dot(left, right, preferred_element_type=F32)


def matmul_rows(left, right):
    return lax.dot_general(left, right, (((1,), (1,)), ((), ())), preferred_element_type=F32)


def matmul_cols(left, right):
    return lax.dot_general(left, right, (((0,), (0,)), ((), ())), preferred_element_type=F32)


def rms_scale(values):
    return lax.rsqrt(jnp.mean(values * values, axis=-1, keepdims=True) + norm_eps)


def rope_tables(length, width):
    position = jnp.arange(length, dtype=F32)
    rates = jnp.exp(jnp.arange(width // 2, dtype=F32) * (-2.0 * math.log(10000.0) / width))
    angle = position[:, None] * rates[None, :]
    return (jnp.cos(angle), jnp.sin(angle))


def rotate(values, cosine, sine):
    half = values.shape[-1] // 2
    first = values[..., :half]
    second = values[..., half:]
    return jnp.concatenate(
        [first * cosine - second * sine, second * cosine + first * sine], axis=-1
    )


def unrotate(grads, cosine, sine):
    half = grads.shape[-1] // 2
    first = grads[..., :half]
    second = grads[..., half:]
    return jnp.concatenate(
        [first * cosine + second * sine, second * cosine - first * sine], axis=-1
    )


def norm_back(grad_hat, hat, scale_rows):
    return scale_rows * (grad_hat - hat * jnp.mean(grad_hat * hat, axis=-1, keepdims=True))


def expert_kernel(
    seqs, cap, tensors, slots, gates, x, og, wgu, wd, out, dgu, dd, xs, gs, parts, backs, acc_gu, acc_d, sems
):
    step = pl.program_id(0)
    width = x.shape[-1]
    half = wd.shape[1]

    @pl.when(step == 0)
    def _():
        acc_gu[...] = jnp.zeros_like(acc_gu)
        acc_d[...] = jnp.zeros_like(acc_d)

    iota = lax.broadcasted_iota(jnp.int32, (cap, SEQ), 0)
    picks = []
    slot_gates = []
    for s in range(seqs):
        chosen = []
        for e in range(EXP_DEV):
            row = s * EXP_DEV + e
            hit = iota == slots[0, row : row + 1, :]
            slot_gates.append(
                jnp.sum(jnp.where(hit, gates[0, row : row + 1, :], 0.0), axis=1, keepdims=True)
            )
            chosen.append(hit.astype(F32).astype(BF))
        picks.append(jnp.concatenate(chosen, axis=0))
    for s in range(seqs):
        for t in range(tensors):
            cols = slice(t * width, (t + 1) * width)
            rows = slice(s * SEQ, (s + 1) * SEQ)
            got = matmul(picks[s], x[0, t, rows, :])
            grad = matmul(picks[s], og[0, t, rows, :])
            for e in range(EXP_DEV):
                xs[e, s * cap : (s + 1) * cap, cols] = got[e * cap : (e + 1) * cap].astype(BF)
                gs[e, s * cap : (s + 1) * cap, cols] = (
                    grad[e * cap : (e + 1) * cap] * slot_gates[s * EXP_DEV + e]
                ).astype(BF)
    for e in range(EXP_DEV):
        gate_col = jnp.concatenate([slot_gates[s * EXP_DEV + e] for s in range(seqs)], axis=0)
        both = matmul(xs[e], wgu[e])
        gated = both[:, :half]
        upper = both[:, half:]
        sig = jax.nn.sigmoid(gated)
        act = gated * sig
        hidden = (act * upper).astype(BF)
        grad_hidden = matmul_rows(gs[e], wd[e])
        grad_gu = jnp.concatenate(
            [
                (grad_hidden * upper * sig * (1.0 + gated * (1.0 - sig))).astype(BF),
                (grad_hidden * act).astype(BF),
            ],
            axis=1,
        )
        part = (matmul(hidden, wd[e]) * gate_col).astype(BF)
        back = matmul_rows(grad_gu, wgu[e]).astype(BF)
        for s in range(seqs):
            parts[s, e * cap : (e + 1) * cap, :] = part[s * cap : (s + 1) * cap]
            backs[s, e * cap : (e + 1) * cap, :] = back[s * cap : (s + 1) * cap]
        acc_d[e] += matmul_cols(hidden, gs[e])
        acc_gu[e] += matmul_cols(xs[e], grad_gu)
    for s in range(seqs):
        for t in range(tensors):
            cols = slice(t * width, (t + 1) * width)
            rows = slice(s * SEQ, (s + 1) * SEQ)
            out[0, t, 0, rows, :] = matmul_cols(picks[s], parts[s, :, cols]).astype(BF)
            out[0, t, 1, rows, :] = matmul_cols(picks[s], backs[s, :, cols]).astype(BF)

    @pl.when(step == pl.num_programs(0) - 1)
    def _():
        first = pltpu.make_async_copy(acc_gu, dgu, sems.at[0])
        second = pltpu.make_async_copy(acc_d, dd, sems.at[1])
        first.start()
        second.start()
        first.wait()
        second.wait()


def run_experts(slots, gates, x, og, wgu, wd, cap):
    groups, tensors, count, width = x.shape
    seqs = count // SEQ
    half = wd.shape[1]
    rows = slots.shape[1]
    stream = lambda g: (g, 0, 0, 0)
    return pl.pallas_call(
        functools.partial(expert_kernel, seqs, cap, tensors),
        grid=(groups,),
        in_specs=[
            pl.BlockSpec((1, rows, SEQ), lambda g: (g, 0, 0)),
            pl.BlockSpec((1, rows, SEQ), lambda g: (g, 0, 0)),
            pl.BlockSpec((1, tensors, count, width), stream),
            pl.BlockSpec((1, tensors, count, width), stream),
            pl.BlockSpec(wgu.shape, lambda g: (0, 0, 0), pipeline_mode=pl.Buffered(1)),
            pl.BlockSpec(wd.shape, lambda g: (0, 0, 0), pipeline_mode=pl.Buffered(1)),
        ],
        out_specs=[
            pl.BlockSpec((1, tensors, 2, count, width), lambda g: (g, 0, 0, 0, 0)),
            pl.BlockSpec(memory_space=pl.ANY),
            pl.BlockSpec(memory_space=pl.ANY),
        ],
        out_shape=[
            jax.ShapeDtypeStruct((groups, tensors, 2, count, width), BF),
            jax.ShapeDtypeStruct(wgu.shape, F32),
            jax.ShapeDtypeStruct(wd.shape, F32),
        ],
        scratch_shapes=[
            pltpu.VMEM((EXP_DEV, seqs * cap, D), BF),
            pltpu.VMEM((EXP_DEV, seqs * cap, D), BF),
            pltpu.VMEM((seqs, EXP_DEV * cap, D), BF),
            pltpu.VMEM((seqs, EXP_DEV * cap, D), BF),
            pltpu.VMEM(wgu.shape, F32),
            pltpu.VMEM(wd.shape, F32),
            pltpu.SemaphoreType.DMA((2,)),
        ],
        compiler_params=pltpu.CompilerParams(
            dimension_semantics=("arbitrary",), vmem_limit_bytes=60 * 1024 * 1024
        ),
        cost_estimate=pl.CostEstimate(
            flops=groups * EXP_DEV * seqs * cap * D * (half * 18 + SEQ * 8),
            bytes_accessed=groups * tensors * count * width * 8 + wgu.size * 9,
            transcendentals=groups * EXP_DEV * seqs * cap * half,
        ),
        name="experts",
    )(slots, gates, x, og, wgu, wd)


def local_wide(
    hidden_in,
    out_grad,
    first_gain,
    query_weight,
    latent_weight,
    latent_gain,
    expand_weight,
    output_weight,
    second_gain,
    shared_gate,
    shared_up,
    shared_down,
    expert_gate,
    expert_up,
    expert_down,
    routes,
    gate_values,
):
    groups = lax.axis_size("expert")
    tensors = lax.axis_size("tensor")
    place = lax.axis_index("tensor")
    mine = lax.axis_index("expert")
    experts_all = EXP_DEV * groups
    cap = SEQ * TOP * 4 // (3 * experts_all)
    width = D // tensors
    heads = H // tensors
    count = hidden_in.shape[0]
    seqs = count // SEQ
    rows_dev = D // groups
    scale = (DN + DR) ** (-0.5)
    cosine, sine = rope_tables(SEQ, DR)
    blocks = jnp.arange(SEQ, dtype=jnp.int32) // BLOCK
    allowed = (blocks[None, :] <= blocks[:, None])[None, None]

    whole_in = lax.all_gather(hidden_in, "tensor", axis=1, tiled=True)
    qc = query_weight.shape[1]
    oc = output_weight.shape[1]
    lc = latent_weight.shape[1]
    sc = shared_gate.shape[1]
    er, ec = expand_weight.shape
    cut = er * ec // rows_dev
    fold = rows_dev // er
    expand_rows = jnp.concatenate(
        [expand_weight[:, i * cut : (i + 1) * cut] for i in range(fold)], axis=0
    )
    attn_all = lax.all_gather(
        jnp.concatenate([query_weight, output_weight, expand_rows, latent_weight], axis=1),
        "expert",
        axis=0,
        tiled=True,
    )
    full_query = attn_all[:, :qc]
    full_output = attn_all[:, qc : qc + oc]
    full_latent = attn_all[:, qc + oc + cut :]
    full_expand = (
        attn_all[:, qc + oc : qc + oc + cut]
        .reshape(groups, fold, er, cut)
        .transpose(0, 2, 1, 3)
        .reshape(groups * er, ec)
    )
    gains = lax.all_gather(
        jnp.concatenate([first_gain, second_gain, latent_gain]).astype(F32), "expert", axis=0
    )
    gain_first = gains[:, :rows_dev].reshape(-1)
    gain_mid = gains[:, rows_dev : 2 * rows_dev].reshape(-1)
    gain_kv = gains[:, 2 * rows_dev :].reshape(-1)
    table = lax.all_gather(
        jnp.concatenate([routes.T.astype(F32), gate_values.T], axis=0), "expert", axis=0
    )
    pieces = max(1, min(seqs, groups // 8))
    per = count // pieces

    def to_all(rows):
        return lax.all_gather(rows, ("expert", "tensor"), axis=0).reshape(
            groups, tensors, per, width
        )

    og_first = to_all(out_grad[:per])
    shared_all = lax.all_gather(
        jnp.concatenate([shared_gate, shared_up, shared_down], axis=1), "expert", axis=0, tiled=True
    )
    full_sgu = shared_all[:, : 2 * sc]
    full_sdown = shared_all[:, 2 * sc :]

    inputs = whole_in.astype(F32)
    first_scale = rms_scale(inputs)
    first_hat = inputs * first_scale
    normed = (first_hat * gain_first).astype(BF)
    query = matmul(normed, full_query).reshape(seqs, SEQ, heads, DN + DR)
    latent = matmul(normed, full_latent)
    compressed = latent[:, :KV_RANK]
    latent_scale = rms_scale(compressed)
    latent_hat = compressed * latent_scale
    latent_normed = (latent_hat * gain_kv).astype(BF)
    expanded = matmul(latent_normed, full_expand).reshape(seqs, SEQ, heads, DN + DV)
    queries = jnp.concatenate(
        [query[..., :DN], rotate(query[..., DN:], cosine[:, None, :], sine[:, None, :])], axis=-1
    ).astype(BF)
    key_rope = rotate(latent[:, KV_RANK:].reshape(seqs, SEQ, DR), cosine, sine).astype(BF)
    keys = jnp.concatenate(
        [
            expanded[..., :DN].astype(BF),
            jnp.broadcast_to(key_rope[:, :, None, :], (seqs, SEQ, heads, DR)),
        ],
        axis=-1,
    )
    values = expanded[..., DN:].astype(BF)
    scores = jnp.where(
        allowed,
        jnp.einsum("nqhc,nkhc->nhqk", queries, keys, preferred_element_type=F32) * scale,
        masked_value,
    )
    peak = jnp.max(scores, axis=-1, keepdims=True)
    log_total = peak + jnp.log(jnp.sum(jnp.exp(scores - peak), axis=-1, keepdims=True))
    weights = jnp.exp(scores - log_total)
    mixed = (
        jnp.einsum("nhqk,nkhc->nqhc", weights.astype(BF), values, preferred_element_type=F32)
        .astype(BF)
        .reshape(count, heads * DV)
    )
    attended = lax.psum(matmul_rows(mixed, full_output).astype(BF), "tensor").astype(F32)
    middle = inputs + attended
    second_scale = rms_scale(middle)
    second_hat = middle * second_scale
    mixer_in = (second_hat * gain_mid).astype(BF)
    mixer_slice = lax.dynamic_slice_in_dim(mixer_in, place * width, width, 1)

    local_experts = (mine * EXP_DEV + jnp.arange(EXP_DEV, dtype=jnp.int32)).astype(F32)
    route_t = table[:, :TOP].reshape(groups, TOP, seqs, SEQ)
    gate_t = table[:, TOP:].reshape(groups, TOP, seqs, SEQ)
    named = route_t[:, :, :, None, :] == local_experts[None, None, None, :, None]
    gate_of = jnp.sum(jnp.where(named, gate_t[:, :, :, None, :], 0.0), axis=1)
    used = jnp.any(named, axis=1)
    before = (
        jnp.arange(SEQ, dtype=jnp.int32)[:, None] < jnp.arange(SEQ, dtype=jnp.int32)[None, :]
    ).astype(BF)
    prior = jnp.einsum("gset,tu->gseu", used.astype(BF), before, preferred_element_type=F32)
    slot_of = jnp.where(used & (prior < cap), prior, -1.0).astype(jnp.int32)
    slot_of = slot_of.reshape(groups, seqs * EXP_DEV, SEQ)
    gate_of = gate_of.reshape(groups, seqs * EXP_DEV, SEQ)

    ff = expert_gate.shape[2]
    half = -(-ff // 128) * 128
    wide = ((0, 0), (0, 0), (0, half - ff))
    wgu = jnp.concatenate([jnp.pad(expert_gate, wide), jnp.pad(expert_up, wide)], axis=2)
    wd = jnp.pad(expert_down, ((0, 0), (0, half - ff), (0, 0)))
    rows = slot_of.shape[1] // pieces
    sums = []
    dgu = dd = None
    for i in range(pieces):
        span = slice(i * per, (i + 1) * per)
        mixer_rows, og_rows = mixer_slice[span], out_grad[span]
        if i > 0:
            mixer_rows, og_rows, *sums = lax.optimization_barrier((mixer_rows, og_rows, *sums))
        outs, g_gu, g_d = run_experts(
            slot_of[:, i * rows : (i + 1) * rows],
            gate_of[:, i * rows : (i + 1) * rows],
            to_all(mixer_rows),
            og_first if i == 0 else to_all(og_rows),
            wgu,
            wd,
            cap,
        )
        dgu = g_gu if dgu is None else dgu + g_gu
        dd = g_d if dd is None else dd + g_d
        summed = lax.psum_scatter(
            outs.reshape(groups * tensors * 2 * per, width),
            ("expert", "tensor"),
            scatter_dimension=0,
            tiled=True,
        )
        sums.append(summed.reshape(2, per, width))
    summed = jnp.concatenate(sums, axis=1) if pieces > 1 else sums[0]
    total_gate = dgu[:, :, :ff]
    total_up = dgu[:, :, half : half + ff]
    total_down = dd[:, :ff]

    if pieces == 1:
        whole_grad = lax.dynamic_slice_in_dim(og_first, mine, 1, 0)[0]
        whole_grad = whole_grad.transpose(1, 0, 2).reshape(count, D)
    else:
        whole_grad = lax.all_gather(out_grad, "tensor", axis=1, tiled=True)
    shared_gu = matmul(mixer_in, full_sgu)
    shared_g = shared_gu[:, :sc]
    shared_u = shared_gu[:, sc:]
    shared_sig = jax.nn.sigmoid(shared_g)
    shared_hidden = (shared_g * shared_sig * shared_u).astype(BF)
    shared_part = matmul_rows(shared_hidden, full_sdown)
    grad_shared = matmul(whole_grad, full_sdown)
    step_sdown = matmul_cols(whole_grad, shared_hidden)
    grad_sg = (grad_shared * shared_u * shared_sig * (1.0 + shared_g * (1.0 - shared_sig))).astype(
        BF
    )
    grad_su = (grad_shared * shared_g * shared_sig).astype(BF)
    grad_sgu = jnp.concatenate([grad_sg, grad_su], axis=1)
    step_sgu = matmul_cols(mixer_in, grad_sgu)
    mixer_part = matmul_rows(grad_sgu, full_sgu)
    shared_sums = lax.psum_scatter(
        jnp.concatenate([shared_part.astype(BF), mixer_part.astype(BF)], axis=0),
        "tensor",
        scatter_dimension=1,
        tiled=True,
    )
    middle_slice = lax.dynamic_slice_in_dim(middle, place * width, width, 1)
    block_out = (
        middle_slice + summed[0].astype(F32) + shared_sums[:count].astype(F32)
    ).astype(BF)
    grad_mixer = lax.all_gather(
        (summed[1].astype(F32) + shared_sums[count:].astype(F32)).astype(BF),
        "tensor",
        axis=1,
        tiled=True,
    ).astype(F32)
    shared_steps = lax.psum_scatter(
        jnp.concatenate([step_sgu.astype(BF), step_sdown.astype(BF)], axis=1),
        "expert",
        scatter_dimension=0,
        tiled=True,
    ).astype(F32)

    step_gain_two = jnp.sum(grad_mixer * second_hat, axis=0)
    grad_middle = whole_grad.astype(F32) + norm_back(
        grad_mixer * gain_mid, second_hat, second_scale
    )
    grad_att = grad_middle.astype(BF)
    step_output = matmul_cols(grad_att, mixed)
    grad_mixed = matmul(grad_att, full_output).astype(BF).reshape(seqs, SEQ, heads, DV)
    grad_weights = jnp.einsum(
        "nqhc,nkhc->nhqk", grad_mixed, values, preferred_element_type=F32
    )
    grad_scores = (
        weights * (grad_weights - jnp.sum(weights * grad_weights, axis=-1, keepdims=True))
    ).astype(BF)
    grad_values = jnp.einsum(
        "nhqk,nqhc->nkhc", weights.astype(BF), grad_mixed, preferred_element_type=F32
    )
    grad_queries = (
        jnp.einsum("nhqk,nkhc->nqhc", grad_scores, keys, preferred_element_type=F32) * scale
    )
    grad_keys = (
        jnp.einsum("nhqk,nqhc->nkhc", grad_scores, queries, preferred_element_type=F32) * scale
    )
    grad_query = (
        jnp.concatenate(
            [
                grad_queries[..., :DN],
                unrotate(grad_queries[..., DN:], cosine[:, None, :], sine[:, None, :]),
            ],
            axis=-1,
        )
        .astype(BF)
        .reshape(count, heads * (DN + DR))
    )
    step_query = matmul_cols(normed, grad_query)
    query_part = matmul_rows(grad_query, full_query)
    rope_part = unrotate(jnp.sum(grad_keys[..., DN:], axis=2), cosine, sine).reshape(count, DR)
    grad_expanded = (
        jnp.concatenate([grad_keys[..., :DN], grad_values], axis=-1)
        .astype(BF)
        .reshape(count, heads * (DN + DV))
    )
    step_expand = matmul_cols(latent_normed, grad_expanded)
    latent_part = matmul_rows(grad_expanded, full_expand)
    latent_sum = lax.psum(
        jnp.concatenate([latent_part.astype(BF), rope_part.astype(BF)], axis=1), "tensor"
    ).astype(F32)
    grad_lnormed = latent_sum[:, :KV_RANK]
    step_gain_latent = jnp.sum(grad_lnormed * latent_hat, axis=0)
    grad_compressed = norm_back(grad_lnormed * gain_kv, latent_hat, latent_scale)
    grad_lat = jnp.concatenate([grad_compressed, latent_sum[:, KV_RANK:]], axis=-1).astype(BF)
    step_latent = matmul_cols(normed, grad_lat)
    query_sum = lax.psum_scatter(
        query_part.astype(BF), "tensor", scatter_dimension=1, tiled=True
    ).astype(F32)
    latent_slice = lax.dynamic_slice_in_dim(full_latent, place * width, width, 0)
    grad_normed = query_sum + matmul_rows(grad_lat, latent_slice)
    first_hat_slice = lax.dynamic_slice_in_dim(first_hat, place * width, width, 1)
    gain_first_slice = lax.dynamic_slice_in_dim(gain_first, place * width, width, 0)
    grad_hat = grad_normed * gain_first_slice
    row_dot = lax.psum(jnp.sum(grad_hat * first_hat_slice, axis=1), "tensor") / D
    grad_middle_slice = lax.dynamic_slice_in_dim(grad_middle, place * width, width, 1)
    input_grad = grad_middle_slice + first_scale * (grad_hat - first_hat_slice * row_dot[:, None])
    step_gain_one = jnp.sum(grad_normed * first_hat_slice, axis=0)

    expand_back = (
        step_expand.astype(BF)
        .reshape(groups, er, fold, cut)
        .transpose(0, 2, 1, 3)
        .reshape(groups * rows_dev, cut)
    )
    attn_steps = lax.psum_scatter(
        jnp.concatenate(
            [step_query.astype(BF), step_output.astype(BF), expand_back, step_latent.astype(BF)],
            axis=1,
        ),
        "expert",
        scatter_dimension=0,
        tiled=True,
    ).astype(F32)
    grad_expand = attn_steps[:, qc + oc : qc + oc + cut]
    grad_expand = jnp.concatenate(
        [grad_expand[i * er : (i + 1) * er] for i in range(fold)], axis=1
    )
    one_full = lax.dynamic_update_slice_in_dim(
        jnp.zeros((D,), F32), step_gain_one, place * width, 0
    )
    gain_sums = lax.psum(
        jnp.concatenate([one_full, step_gain_two / tensors, step_gain_latent / tensors]),
        ("expert", "tensor"),
    )
    kv_dev = latent_gain.shape[0]
    return (
        block_out,
        input_grad,
        lax.dynamic_slice_in_dim(gain_sums, mine * rows_dev, rows_dev, 0),
        attn_steps[:, :qc],
        attn_steps[:, qc + oc + cut :],
        lax.dynamic_slice_in_dim(gain_sums, 2 * D + mine * kv_dev, kv_dev, 0),
        grad_expand,
        attn_steps[:, qc : qc + oc],
        lax.dynamic_slice_in_dim(gain_sums, D + mine * rows_dev, rows_dev, 0),
        shared_steps[:, :sc],
        shared_steps[:, sc : 2 * sc],
        shared_steps[:, 2 * sc :],
        total_gate,
        total_up,
        total_down,
    )


def group_kernel(
    k,
    xr,
    seqs,
    cap,
    slots, gates, mx_own, mx_peer, og_all, wgu, wd, shared,
    s_xs, s_gs, s_gu, s_hid,
    back_keep, back_send, rout_keep, rout_send, d_shared, o_xs, o_gs, o_gu, o_hid,
    full_x, og, full_og, xs, gs, parts, backs, hid_s, gu_s, sem,
):
    del s_xs, s_gs, s_gu, s_hid
    e = pl.program_id(0)
    place = lax.axis_index("tensor")
    mine = lax.axis_index("expert")
    ring = lax.axis_size("expert") // 2
    group = lax.rem(mine // 2 + ring - k, ring) * 2 + jnp.bitwise_xor(lax.rem(mine, 2), xr)
    width = og_all.shape[-1]
    half = wd.shape[1]
    units = shared.shape[0] // 3

    def cols_of(rel):
        return pl.ds(pl.multiple_of(jnp.bitwise_xor(place, rel) * width, width), width)

    iota = lax.broadcasted_iota(jnp.int32, (cap, SEQ), 0)

    def pick_of(s):
        chosen = []
        for j in range(EXP_DEV):
            row = s * EXP_DEV + j
            chosen.append((iota == slots[group, row : row + 1, :]).astype(F32).astype(BF))
        return jnp.concatenate(chosen, axis=0)

    def gate_of(s, j):
        row = s * EXP_DEV + j
        hit = iota == slots[group, pl.ds(row, 1), :]
        return jnp.sum(jnp.where(hit, gates[group, pl.ds(row, 1), :], 0.0), axis=1, keepdims=True)

    @pl.when(e == 0)
    def _():
        fetch = pltpu.make_async_copy(og_all.at[group], og, sem)
        fetch.start()
        for rel, ref in ((0, mx_own.at[0]), (2, mx_own.at[1]), (1, mx_peer.at[0]), (3, mx_peer.at[1])):
            full_x[:, cols_of(rel)] = ref[...]
        fetch.wait()
        for t in range(D // width):
            full_og[:, t * width : (t + 1) * width] = og[t]
        for s in range(seqs):
            pick = pick_of(s)
            gate_cols = [gate_of(s, j) for j in range(EXP_DEV)]
            rows = slice(s * SEQ, (s + 1) * SEQ)
            for c in range(D // width):
                cols = slice(c * width, (c + 1) * width)
                got = matmul(pick, full_x[rows, cols])
                grad = matmul(pick, full_og[rows, cols])
                for j in range(EXP_DEV):
                    here = slice(s * cap, (s + 1) * cap)
                    xs[j, here, cols] = got[j * cap : (j + 1) * cap].astype(BF)
                    gs[j, here, cols] = (grad[j * cap : (j + 1) * cap] * gate_cols[j]).astype(BF)
        both = matmul_rows(full_x[...], shared[: 2 * units])
        gated = both[:, :units]
        upper = both[:, units:]
        sig = jax.nn.sigmoid(gated)
        act = gated * sig
        grad = matmul_rows(full_og[...], shared[2 * units :])
        hid_s[...] = (act * upper).astype(BF)
        gu_s[:, :units] = (grad * upper * sig * (1.0 + gated * (1.0 - sig))).astype(BF)
        gu_s[:, units:] = (grad * act).astype(BF)
        d_shared[: 2 * units] = matmul_cols(gu_s[...], full_x[...])
        d_shared[2 * units :] = matmul_cols(hid_s[...], full_og[...])

    x_rows = xs[e]
    g_rows = gs[e]
    both = matmul(x_rows, wgu[0])
    gated = both[:, :half]
    upper = both[:, half:]
    sig = jax.nn.sigmoid(gated)
    act = gated * sig
    hidden = (act * upper).astype(BF)
    grad_hidden = matmul_rows(g_rows, wd[0])
    grad_gu = jnp.concatenate(
        [
            (grad_hidden * upper * sig * (1.0 + gated * (1.0 - sig))).astype(BF),
            (grad_hidden * act).astype(BF),
        ],
        axis=1,
    )
    o_xs[0, 0] = x_rows
    o_gs[0, 0] = g_rows
    o_gu[0, 0] = grad_gu
    o_hid[0, 0] = hidden
    gate_col = jnp.concatenate([gate_of(s, e) for s in range(seqs)], axis=0)
    part = (matmul(hidden, wd[0]) * gate_col).astype(BF)
    back = matmul_rows(grad_gu, wgu[0]).astype(BF)
    for s in range(seqs):
        here = pl.ds(pl.multiple_of(e * cap, cap), cap)
        parts[s, here, :] = part[s * cap : (s + 1) * cap]
        backs[s, here, :] = back[s * cap : (s + 1) * cap]

    @pl.when(e == EXP_DEV - 1)
    def _():
        for s in range(seqs):
            pick = pick_of(s)
            rows = slice(s * SEQ, (s + 1) * SEQ)
            for rel, b_ref, r_ref, at in (
                (0, back_keep, rout_keep, 0),
                (2, back_keep, rout_keep, 1),
                (1, back_send, rout_send, 0),
                (3, back_send, rout_send, 1),
            ):
                cols = cols_of(rel)
                b_ref[at, rows, :] = (
                    matmul_cols(pick, backs[s, :, cols])
                    + matmul(gu_s[rows, :], shared[: 2 * units, cols])
                ).astype(BF)
                r_ref[at, rows, :] = (
                    matmul_cols(pick, parts[s, :, cols])
                    + matmul(hid_s[rows, :], shared[2 * units :, cols])
                ).astype(BF)


def run_group(k, xr, cap, slots, gates, mx, og, wgu, wd, shared, saved):
    count, width = og.shape[-2:]
    seqs = count // SEQ
    half = wd.shape[1]
    units = shared.shape[0] // 3
    call = k * 2 + xr
    groups = slots.shape[0]
    whole = lambda shape: pl.BlockSpec(shape, lambda e: (0,) * len(shape))
    slab = lambda last: pl.BlockSpec((1, 1, seqs * cap, last), lambda e: (e, call, 0, 0))
    hbm = pl.BlockSpec(memory_space=pl.ANY)
    slab_shape = lambda last: jax.ShapeDtypeStruct((EXP_DEV, groups, seqs * cap, last), BF)
    pair = jax.ShapeDtypeStruct((2, count, width), BF)
    first = 8
    args = [slots, gates, *mx, og, wgu, wd, shared]
    aliases = {}
    if saved is None:
        saved = [jnp.zeros((8, 128), BF)] * 4
    else:
        aliases = {first + i: 5 + i for i in range(4)}
    return pl.pallas_call(
        functools.partial(group_kernel, k, xr, seqs, cap),
        grid=(EXP_DEV,),
        in_specs=[
            whole(slots.shape),
            whole(gates.shape),
            whole((2, count, width)),
            whole((2, count, width)),
            hbm,
            pl.BlockSpec((1, D, 2 * half), lambda e: (e, 0, 0)),
            pl.BlockSpec((1, half, D), lambda e: (e, 0, 0)),
            whole(shared.shape),
            hbm, hbm, hbm, hbm,
        ],
        out_specs=[
            whole((2, count, width)),
            whole((2, count, width)),
            whole((2, count, width)),
            whole((2, count, width)),
            whole((3 * units, D)),
            slab(D),
            slab(D),
            slab(2 * half),
            slab(half),
        ],
        out_shape=[
            pair, pair, pair, pair,
            jax.ShapeDtypeStruct((3 * units, D), F32),
            slab_shape(D), slab_shape(D), slab_shape(2 * half), slab_shape(half),
        ],
        scratch_shapes=[
            pltpu.VMEM((count, D), BF),
            pltpu.VMEM((D // width, count, width), BF),
            pltpu.VMEM((count, D), BF),
            pltpu.VMEM((EXP_DEV, seqs * cap, D), BF),
            pltpu.VMEM((EXP_DEV, seqs * cap, D), BF),
            pltpu.VMEM((seqs, EXP_DEV * cap, D), BF),
            pltpu.VMEM((seqs, EXP_DEV * cap, D), BF),
            pltpu.VMEM((count, units), BF),
            pltpu.VMEM((count, 2 * units), BF),
            pltpu.SemaphoreType.DMA,
        ],
        input_output_aliases=aliases,
        compiler_params=pltpu.CompilerParams(
            dimension_semantics=("arbitrary",), vmem_limit_bytes=60 * 1024 * 1024
        ),
        cost_estimate=pl.CostEstimate(
            flops=EXP_DEV * seqs * cap * D * (half * 12 + SEQ * 8),
            bytes_accessed=40 * 1024 * 1024,
            transcendentals=EXP_DEV * seqs * cap * half,
        ),
        name=f"group_{k}_{xr}",
    )(*args, *saved)


def weight_kernel(xs, gs, gu, hid, d_gate, d_up, d_down, acc_gu, acc_d):
    g = pl.program_id(1)
    ff = d_gate.shape[-1]
    half = hid.shape[-1]

    @pl.when(g == 0)
    def _():
        acc_gu[...] = jnp.zeros_like(acc_gu)
        acc_d[...] = jnp.zeros_like(acc_d)

    for i in range(xs.shape[1]):
        acc_gu[...] += matmul_cols(xs[0, i], gu[0, i])
        acc_d[...] += matmul_cols(hid[0, i], gs[0, i])

    @pl.when(g == pl.num_programs(1) - 1)
    def _():
        d_gate[0] = acc_gu[:, :ff]
        d_up[0] = acc_gu[:, half : half + ff]
        d_down[0] = acc_d[:ff]


def weight_grads(xs, gs, gu, hid, ff):
    groups, rows = xs.shape[1:3]
    half = hid.shape[-1]
    step = 2
    slab = lambda last: pl.BlockSpec((1, step, rows, last), lambda e, g: (e, g, 0, 0))
    out = lambda *dims: pl.BlockSpec((1, *dims), lambda e, g: (e, 0, 0))
    return pl.pallas_call(
        weight_kernel,
        grid=(EXP_DEV, groups // step),
        in_specs=[slab(D), slab(D), slab(2 * half), slab(half)],
        out_specs=[out(D, ff), out(D, ff), out(ff, D)],
        out_shape=[
            jax.ShapeDtypeStruct((EXP_DEV, D, ff), F32),
            jax.ShapeDtypeStruct((EXP_DEV, D, ff), F32),
            jax.ShapeDtypeStruct((EXP_DEV, ff, D), F32),
        ],
        scratch_shapes=[pltpu.VMEM((D, 2 * half), F32), pltpu.VMEM((half, D), F32)],
        compiler_params=pltpu.CompilerParams(
            dimension_semantics=("arbitrary", "arbitrary"), vmem_limit_bytes=60 * 1024 * 1024
        ),
        cost_estimate=pl.CostEstimate(
            flops=EXP_DEV * groups * rows * D * half * 6,
            bytes_accessed=64 * 1024 * 1024,
            transcendentals=0,
        ),
        name="weight_grads",
    )(xs, gs, gu, hid)


def place_kernel(targets, n, *refs):
    blocks, out, sems = refs[:n], refs[n], refs[n + 1]
    copies = [
        pltpu.make_async_copy(block, out.at[target()], sems.at[i])
        for i, (block, target) in enumerate(zip(blocks, targets))
    ]
    for copy in copies:
        copy.start()
    for copy in copies:
        copy.wait()


def place(blocks, targets, count):
    n = len(blocks)
    return pl.pallas_call(
        functools.partial(place_kernel, targets, n),
        in_specs=[pl.BlockSpec(memory_space=pltpu.VMEM)] * n,
        out_specs=pl.BlockSpec(memory_space=pl.ANY),
        out_shape=jax.ShapeDtypeStruct((count, *blocks[0].shape), blocks[0].dtype),
        scratch_shapes=[pltpu.SemaphoreType.DMA((n,))],
        compiler_params=pltpu.CompilerParams(vmem_limit_bytes=16 * 1024 * 1024),
        name="place",
    )(*blocks)


def flip_tensor(x, mask):
    size = lax.axis_size("tensor")
    return lax.ppermute(x, "tensor", [(i, i ^ mask) for i in range(size)])


def to_core(x):
    return flip_tensor(x, 1)


def to_y(x):
    return flip_tensor(x, 2)


def to_x(x):
    size = lax.axis_size("expert")
    return lax.ppermute(x, "expert", [(i, i ^ 1) for i in range(size)])


def to_z(x):
    size = lax.axis_size("expert")
    return lax.ppermute(x, "expert", [(i, (i + 2) % size) for i in range(size)])


def after(x, done):
    return lax.optimization_barrier((x, done))[0]


def add(*terms):
    total = terms[0].astype(F32)
    for term in terms[1:]:
        total = total + term.astype(F32)
    return total.astype(BF)


def gather_pairs(block):
    ring = lax.axis_size("expert") // 2
    pairs = []
    for k in range(ring):
        pairs.append((block, to_x(block)))
        if k < ring - 1:
            block = to_z(block)
    return pairs


def group_at(k, xr):
    def target():
        mine = lax.axis_index("expert")
        ring = lax.axis_size("expert") // 2
        return lax.rem(mine // 2 + ring - k, ring) * 2 + jnp.bitwise_xor(lax.rem(mine, 2), xr)

    return target


def gather_rows(block):
    groups = lax.axis_size("expert")
    pairs = gather_pairs(block)
    blocks = [b for pair in pairs for b in pair]
    targets = [group_at(k, xr) for k in range(groups // 2) for xr in range(2)]
    return place(blocks, targets, groups)


def ring_sum(totals):
    ring = len(totals)
    moving = totals[1]()
    for k in range(2, ring):
        moving = add(to_z(moving), totals[k]())
    return to_z(moving), totals[0]()


def scatter_rows(blocks):
    ring = lax.axis_size("expert") // 2
    at = lambda k, xr: lax.dynamic_index_in_dim(blocks, group_at(k, xr)(), 0, keepdims=False)
    came = {}
    last = None
    for k in [*range(1, ring), 0]:
        sent = at(k, 1)
        if last is not None:
            sent = after(sent, last)
        last = to_x(sent)
        came[k] = last
    return ring_sum([lambda k=k: add(at(k, 0), came[k]) for k in range(ring)])


def pieces_of(x):
    other = to_y(x)
    return x, other, to_core(x), to_core(other)


def join(pieces, axis):
    place_t = lax.axis_index("tensor")
    low_y = place_t // 2 == 0
    low_c = lax.rem(place_t, 2) == 0
    o0, o2, o1, o3 = pieces
    a = (jnp.where(low_y, o0, o2), jnp.where(low_y, o2, o0))
    b = (jnp.where(low_y, o1, o3), jnp.where(low_y, o3, o1))
    out = []
    for y in range(2):
        out += [jnp.where(low_c, a[y], b[y]), jnp.where(low_c, b[y], a[y])]
    return jnp.concatenate(out, axis=axis)


def scatter_cols(x):
    place_t = lax.axis_index("tensor")
    rows = x.shape[0]
    view = x.reshape(rows, 2, 2, -1)
    low_y = place_t // 2 == 0
    low_c = lax.rem(place_t, 2) == 0
    keep = jnp.where(low_c, view[:, :, 0], view[:, :, 1])
    send = jnp.where(low_c, view[:, :, 1], view[:, :, 0])
    half = add(keep, to_core(send))
    mine = jnp.where(low_y, half[:, 0], half[:, 1])
    theirs = jnp.where(low_y, half[:, 1], half[:, 0])
    return mine, to_y(theirs)


def sum_cols(x):
    place_t = lax.axis_index("tensor")
    rows = x.shape[0]
    view = x.reshape(rows, 2, 2, -1)
    low_c = lax.rem(place_t, 2) == 0
    keep = jnp.where(low_c, view[:, :, 0], view[:, :, 1])
    send = jnp.where(low_c, view[:, :, 1], view[:, :, 0])
    half = add(keep, to_core(send))
    half = add(half, to_y(half))
    other = to_core(half)
    return jnp.stack(
        [jnp.where(low_c, half, other), jnp.where(low_c, other, half)], axis=2
    ).reshape(rows, -1)


def small_sum(x):
    x = x + to_core(x)
    return x + to_y(x)


def local(
    hidden_in,
    out_grad,
    first_gain,
    query_weight,
    latent_weight,
    latent_gain,
    expand_weight,
    output_weight,
    second_gain,
    shared_gate,
    shared_up,
    shared_down,
    expert_gate,
    expert_up,
    expert_down,
    routes,
    gate_values,
):
    groups = lax.axis_size("expert")
    tensors = lax.axis_size("tensor")
    ring = groups // 2
    place_t = lax.axis_index("tensor")
    mine = lax.axis_index("expert")
    experts_all = EXP_DEV * groups
    cap = SEQ * TOP * 4 // (3 * experts_all)
    width = D // tensors
    heads = H // tensors
    count = hidden_in.shape[0]
    seqs = count // SEQ
    rows_dev = D // groups
    scale = (DN + DR) ** (-0.5)
    cosine, sine = rope_tables(SEQ, DR)
    blocks = jnp.arange(SEQ, dtype=jnp.int32) // BLOCK
    allowed = (blocks[None, :] <= blocks[:, None])[None, None]
    qc = query_weight.shape[1]
    oc = output_weight.shape[1]
    lc = latent_weight.shape[1]
    sc = shared_gate.shape[1]
    er, ec = expand_weight.shape
    kv_dev = latent_gain.shape[0]
    cut = er * ec // rows_dev
    fold = rows_dev // er
    quarter = rows_dev // tensors

    gain_row = jnp.concatenate([first_gain, second_gain, latent_gain]).reshape(1, -1)
    lat_rows = lax.dynamic_slice_in_dim(latent_weight, place_t * quarter, quarter, 0)
    lat_all = gather_rows(jnp.concatenate([lat_rows, gain_row], axis=0))
    gains = lat_all[:, quarter].astype(F32)
    gain_first = gains[:, :rows_dev].reshape(-1)
    gain_mid = gains[:, rows_dev : 2 * rows_dev].reshape(-1)
    gain_kv = gains[:, 2 * rows_dev :].reshape(-1)
    full_latent = join(pieces_of(lat_all[:, :quarter]), 1).reshape(D, lc)
    expand_rows = jnp.concatenate(
        [expand_weight[:, i * cut : (i + 1) * cut] for i in range(fold)], axis=0
    )
    qe_all = gather_rows(jnp.concatenate([query_weight, output_weight, expand_rows], axis=1))
    full_query = qe_all[:, :, :qc].reshape(D, qc)
    full_expand = (
        qe_all[:, :, qc + oc :].reshape(groups, fold, er, cut).transpose(0, 2, 1, 3).reshape(groups * er, ec)
    )
    full_output = qe_all[:, :, qc : qc + oc].reshape(D, oc)

    units = sc // groups
    wide_units = -(-units // 128) * 128
    shared_t = jnp.stack([shared_gate.T, shared_up.T, shared_down.T]).reshape(3, groups, units, rows_dev)
    shared_t = shared_t.transpose(1, 0, 2, 3).reshape(groups, 3 * units, rows_dev)
    shared_t = lax.all_to_all(shared_t, "expert", split_axis=0, concat_axis=0, tiled=True)
    shared_t = shared_t.reshape(groups, 3, units, rows_dev).transpose(1, 2, 0, 3).reshape(3, units, D)
    shared_w = jnp.pad(shared_t, ((0, 0), (0, wide_units - units), (0, 0))).reshape(3 * wide_units, D)

    table = gather_rows(jnp.concatenate([routes.T.astype(F32), gate_values.T], axis=0))
    og_all = lax.all_gather(out_grad, ("expert", "tensor"), axis=0)
    og_all = og_all.reshape(groups, tensors, count, width)
    whole_grad = lax.dynamic_index_in_dim(og_all, mine, 0, keepdims=False)
    whole_grad = whole_grad.transpose(1, 0, 2).reshape(count, D)

    whole_in = join(pieces_of(hidden_in), 1)
    inputs = whole_in.astype(F32)
    first_scale = rms_scale(inputs)
    first_hat = inputs * first_scale
    normed = (first_hat * gain_first).astype(BF)
    query = matmul(normed, full_query).reshape(seqs, SEQ, heads, DN + DR)
    latent = matmul(normed, full_latent)
    compressed = latent[:, :KV_RANK]
    latent_scale = rms_scale(compressed)
    latent_hat = compressed * latent_scale
    latent_normed = (latent_hat * gain_kv).astype(BF)
    expanded = matmul(latent_normed, full_expand).reshape(seqs, SEQ, heads, DN + DV)
    queries = jnp.concatenate(
        [query[..., :DN], rotate(query[..., DN:], cosine[:, None, :], sine[:, None, :])], axis=-1
    ).astype(BF)
    key_rope = rotate(latent[:, KV_RANK:].reshape(seqs, SEQ, DR), cosine, sine).astype(BF)
    keys = jnp.concatenate(
        [
            expanded[..., :DN].astype(BF),
            jnp.broadcast_to(key_rope[:, :, None, :], (seqs, SEQ, heads, DR)),
        ],
        axis=-1,
    )
    values = expanded[..., DN:].astype(BF)
    scores = jnp.where(
        allowed,
        jnp.einsum("nqhc,nkhc->nhqk", queries, keys, preferred_element_type=F32) * scale,
        masked_value,
    )
    peak = jnp.max(scores, axis=-1, keepdims=True)
    log_total = peak + jnp.log(jnp.sum(jnp.exp(scores - peak), axis=-1, keepdims=True))
    weights = jnp.exp(scores - log_total)
    mixed = (
        jnp.einsum("nhqk,nkhc->nqhc", weights.astype(BF), values, preferred_element_type=F32)
        .astype(BF)
        .reshape(count, heads * DV)
    )
    attended = sum_cols(matmul_rows(mixed, full_output).astype(BF)).astype(F32)
    middle = inputs + attended
    second_scale = rms_scale(middle)
    second_hat = middle * second_scale
    mixer_in = (second_hat * gain_mid).astype(BF)
    low_y = place_t // 2 == 0
    low_c = lax.rem(place_t, 2) == 0
    view = mixer_in.reshape(count, 2, 2, width)
    view = jnp.where(low_c, view[:, :, 0], view[:, :, 1])
    mixer_half = jnp.stack(
        [jnp.where(low_y, view[:, 0], view[:, 1]), jnp.where(low_y, view[:, 1], view[:, 0])]
    )
    mixer_pairs = gather_pairs(mixer_half)

    local_experts = (mine * EXP_DEV + jnp.arange(EXP_DEV, dtype=jnp.int32)).astype(F32)
    route_t = table[:, :TOP].reshape(groups, TOP, seqs, SEQ)
    gate_t = table[:, TOP:].reshape(groups, TOP, seqs, SEQ)
    named = route_t[:, :, :, None, :] == local_experts[None, None, None, :, None]
    gate_of = jnp.sum(jnp.where(named, gate_t[:, :, :, None, :], 0.0), axis=1)
    used = jnp.any(named, axis=1)
    before = (
        jnp.arange(SEQ, dtype=jnp.int32)[:, None] < jnp.arange(SEQ, dtype=jnp.int32)[None, :]
    ).astype(BF)
    prior = jnp.einsum("gset,tu->gseu", used.astype(BF), before, preferred_element_type=F32)
    slot_of = jnp.where(used & (prior < cap), prior, -1.0).astype(jnp.int32)
    slot_of = slot_of.reshape(groups, seqs * EXP_DEV, SEQ)
    gate_of = gate_of.reshape(groups, seqs * EXP_DEV, SEQ)

    ff = expert_gate.shape[2]
    half = -(-ff // 128) * 128
    wide = ((0, 0), (0, 0), (0, half - ff))
    wgu = jnp.concatenate([jnp.pad(expert_gate, wide), jnp.pad(expert_up, wide)], axis=2)
    wd = jnp.pad(expert_down, ((0, 0), (0, half - ff), (0, 0)))
    saved = None
    outs = {}
    d_shared = []
    for k in range(ring):
        for xr in range(2):
            rows = mixer_pairs[k][xr]
            *out, d_sh, s0, s1, s2, s3 = run_group(
                k, xr, cap, slot_of, gate_of, (rows, to_core(rows)), og_all, wgu, wd, shared_w, saved
            )
            saved = [s0, s1, s2, s3]
            outs[k, xr] = out
            d_shared.append(d_sh)

    def over_tensor(keep, send):
        came = to_core(send)
        return add(keep[0], came[0], to_y(add(keep[1], came[1])))

    def combine(at):
        def total(k):
            other = over_tensor(outs[k, 1][at], outs[k, 1][at + 1])
            return add(over_tensor(outs[k, 0][at], outs[k, 0][at + 1]), to_x(other))

        return ring_sum([functools.partial(total, k) for k in range(ring)])

    back_sum = add(*combine(0))
    rout_sum = combine(2)
    total_gate, total_up, total_down = weight_grads(*saved, ff)
    middle_slice = lax.dynamic_slice_in_dim(middle, place_t * width, width, 1)
    block_out = (
        middle_slice + rout_sum[0].astype(F32) + rout_sum[1].astype(F32)
    ).astype(BF)
    shared_step = d_shared[0]
    for term in d_shared[1:]:
        shared_step = shared_step + term
    shared_step = shared_step.reshape(3, wide_units, groups, rows_dev)[:, :units].astype(BF)
    shared_step = shared_step.transpose(2, 0, 1, 3).reshape(groups, 3 * units, rows_dev)
    shared_step = lax.all_to_all(shared_step, "expert", split_axis=0, concat_axis=0, tiled=True)
    shared_step = shared_step.reshape(groups, 3, units, rows_dev).transpose(1, 3, 0, 2)
    shared_step = shared_step.reshape(3, rows_dev, sc).astype(F32)

    grad_mixer = join(pieces_of(back_sum), 1).astype(F32)
    step_gain_two = jnp.sum(grad_mixer * second_hat, axis=0)
    grad_middle = whole_grad.astype(F32) + norm_back(
        grad_mixer * gain_mid, second_hat, second_scale
    )
    grad_att = grad_middle.astype(BF)
    step_output = matmul_cols(grad_att, mixed)
    output_sum = scatter_rows(step_output.astype(BF).reshape(groups, rows_dev, -1))
    grad_mixed = matmul(grad_att, full_output).astype(BF).reshape(seqs, SEQ, heads, DV)
    grad_weights = jnp.einsum(
        "nqhc,nkhc->nhqk", grad_mixed, values, preferred_element_type=F32
    )
    grad_scores = (
        weights * (grad_weights - jnp.sum(weights * grad_weights, axis=-1, keepdims=True))
    ).astype(BF)
    grad_values = jnp.einsum(
        "nhqk,nqhc->nkhc", weights.astype(BF), grad_mixed, preferred_element_type=F32
    )
    grad_queries = (
        jnp.einsum("nhqk,nkhc->nqhc", grad_scores, keys, preferred_element_type=F32) * scale
    )
    grad_keys = (
        jnp.einsum("nhqk,nqhc->nkhc", grad_scores, queries, preferred_element_type=F32) * scale
    )
    grad_query = (
        jnp.concatenate(
            [
                grad_queries[..., :DN],
                unrotate(grad_queries[..., DN:], cosine[:, None, :], sine[:, None, :]),
            ],
            axis=-1,
        )
        .astype(BF)
        .reshape(count, heads * (DN + DR))
    )
    step_query = matmul_cols(normed, grad_query)
    query_part = matmul_rows(grad_query, full_query)
    rope_part = unrotate(jnp.sum(grad_keys[..., DN:], axis=2), cosine, sine).reshape(count, DR)
    grad_expanded = (
        jnp.concatenate([grad_keys[..., :DN], grad_values], axis=-1)
        .astype(BF)
        .reshape(count, heads * (DN + DV))
    )
    step_expand = matmul_cols(latent_normed, grad_expanded)
    expand_back = (
        step_expand.astype(BF)
        .reshape(groups, er, fold, cut)
        .transpose(0, 2, 1, 3)
        .reshape(groups * rows_dev, cut)
    )
    qe_sum = scatter_rows(
        jnp.concatenate([step_query.astype(BF), expand_back], axis=1).reshape(groups, rows_dev, -1)
    )
    latent_part = matmul_rows(grad_expanded, full_expand)
    lat_part = jnp.concatenate([latent_part, rope_part], axis=1).astype(BF)
    lat_part = add(lat_part, to_core(lat_part))
    latent_sum = lat_part.astype(F32) + to_y(lat_part).astype(F32)
    grad_lnormed = latent_sum[:, :KV_RANK]
    step_gain_latent = jnp.sum(grad_lnormed * latent_hat, axis=0)
    grad_compressed = norm_back(grad_lnormed * gain_kv, latent_hat, latent_scale)
    grad_lat = jnp.concatenate([grad_compressed, latent_sum[:, KV_RANK:]], axis=-1).astype(BF)
    query_sum = scatter_cols(query_part.astype(BF))
    latent_slice = lax.dynamic_slice_in_dim(full_latent, place_t * width, width, 0)
    grad_normed = (
        query_sum[0].astype(F32) + query_sum[1].astype(F32) + matmul_rows(grad_lat, latent_slice)
    )
    first_hat_slice = lax.dynamic_slice_in_dim(first_hat, place_t * width, width, 1)
    gain_first_slice = lax.dynamic_slice_in_dim(gain_first, place_t * width, width, 0)
    grad_hat = grad_normed * gain_first_slice
    row_dot = small_sum(jnp.sum(grad_hat * first_hat_slice, axis=1).reshape(-1, 128)) / D
    grad_middle_slice = lax.dynamic_slice_in_dim(grad_middle, place_t * width, width, 1)
    input_grad = grad_middle_slice + first_scale * (
        grad_hat - first_hat_slice * row_dot.reshape(-1, 1)
    )
    step_gain_one = jnp.sum(grad_normed * first_hat_slice, axis=0)

    normed_part = lax.dynamic_index_in_dim(
        normed.reshape(count, groups, tensors, quarter), place_t, 2, keepdims=False
    ).reshape(count, groups * quarter)
    step_latent = matmul_cols(normed_part, grad_lat).reshape(groups, quarter, lc)
    one_full = lax.dynamic_update_slice_in_dim(
        jnp.zeros((D,), F32), step_gain_one, place_t * width, 0
    )
    once = jnp.where(place_t == 0, 1.0, 0.0)
    gain_rows = jnp.concatenate(
        [
            one_full.reshape(groups, rows_dev),
            (step_gain_two * once).reshape(groups, rows_dev),
            (step_gain_latent * once).reshape(groups, kv_dev),
        ],
        axis=1,
    )
    lat_sum = add(
        *scatter_rows(jnp.concatenate([step_latent, gain_rows[:, None]], axis=1).astype(BF))
    )
    lat_pieces = pieces_of(lat_sum)
    gain_sum = sum(piece[quarter].astype(F32) for piece in lat_pieces)
    grad_latent = join([piece[:quarter] for piece in lat_pieces], 0).astype(F32)
    qe = qe_sum[0].astype(F32) + qe_sum[1].astype(F32)
    grad_expand = jnp.concatenate(
        [qe[i * er : (i + 1) * er, qc:] for i in range(fold)], axis=1
    )
    return (
        block_out,
        input_grad,
        gain_sum[:rows_dev],
        qe[:, :qc],
        grad_latent,
        gain_sum[2 * rows_dev :],
        grad_expand,
        output_sum[0].astype(F32) + output_sum[1].astype(F32),
        gain_sum[rows_dev : 2 * rows_dev],
        shared_step[0],
        shared_step[1],
        shared_step[2],
        total_gate,
        total_up,
        total_down,
    )


def solution(mesh):
    body = local if mesh.shape["expert"] == 8 and mesh.shape["tensor"] == 4 else local_wide
    both = P("expert", "tensor")
    cols = P("expert", None, "tensor")
    rows = P("expert", "tensor", None)
    one = P("expert")
    flat = P("expert", None)
    return jax.shard_map(
        body,
        mesh=mesh,
        in_specs=(
            both, both, one, both, flat, one, both, both, one, both, both, both,
            cols, cols, rows, flat, flat,
        ),
        out_specs=(
            both, both, one, both, flat, one, both, both, one, both, both, both,
            cols, cols, rows,
        ),
        check_vma=False,
    )
```

```python
import functools
import math

import jax
import jax.numpy as jnp
from jax import lax
from jax.experimental import pallas as pl
from jax.experimental.pallas import tpu as pltpu
from jax.sharding import PartitionSpec as P

D = 2048
H = 16
DN = 128
DR = 64
DV = 128
KV_RANK = 512
TOP = 6
EXP_DEV = 2
SEQ = 256
BLOCK = 128

norm_eps = 1e-06
masked_value = -1000000000.0
BF = jnp.bfloat16
F32 = jnp.float32


def matmul(left, right):
    return jnp.dot(left, right, preferred_element_type=F32)


def matmul_rows(left, right):
    return lax.dot_general(left, right, (((1,), (1,)), ((), ())), preferred_element_type=F32)


def matmul_cols(left, right):
    return lax.dot_general(left, right, (((0,), (0,)), ((), ())), preferred_element_type=F32)


def rms_scale(values):
    return lax.rsqrt(jnp.mean(values * values, axis=-1, keepdims=True) + norm_eps)


def rope_tables(length, width):
    position = jnp.arange(length, dtype=F32)
    rates = jnp.exp(jnp.arange(width // 2, dtype=F32) * (-2.0 * math.log(10000.0) / width))
    angle = position[:, None] * rates[None, :]
    return (jnp.cos(angle), jnp.sin(angle))


def rotate(values, cosine, sine):
    half = values.shape[-1] // 2
    first = values[..., :half]
    second = values[..., half:]
    return jnp.concatenate(
        [first * cosine - second * sine, second * cosine + first * sine], axis=-1
    )


def unrotate(grads, cosine, sine):
    half = grads.shape[-1] // 2
    first = grads[..., :half]
    second = grads[..., half:]
    return jnp.concatenate(
        [first * cosine + second * sine, second * cosine - first * sine], axis=-1
    )


def norm_back(grad_hat, hat, scale_rows):
    return scale_rows * (grad_hat - hat * jnp.mean(grad_hat * hat, axis=-1, keepdims=True))


def expert_kernel(
    seqs, cap, tensors, slots, gates, x, og, wgu, wd, out, dgu, dd, xs, gs, parts, backs, acc_gu, acc_d, sems
):
    step = pl.program_id(0)
    width = x.shape[-1]
    half = wd.shape[1]

    @pl.when(step == 0)
    def _():
        acc_gu[...] = jnp.zeros_like(acc_gu)
        acc_d[...] = jnp.zeros_like(acc_d)

    iota = lax.broadcasted_iota(jnp.int32, (cap, SEQ), 0)
    picks = []
    slot_gates = []
    for s in range(seqs):
        chosen = []
        for e in range(EXP_DEV):
            row = s * EXP_DEV + e
            hit = iota == slots[0, row : row + 1, :]
            slot_gates.append(
                jnp.sum(jnp.where(hit, gates[0, row : row + 1, :], 0.0), axis=1, keepdims=True)
            )
            chosen.append(hit.astype(F32).astype(BF))
        picks.append(jnp.concatenate(chosen, axis=0))
    for s in range(seqs):
        for t in range(tensors):
            cols = slice(t * width, (t + 1) * width)
            rows = slice(s * SEQ, (s + 1) * SEQ)
            got = matmul(picks[s], x[0, t, rows, :])
            grad = matmul(picks[s], og[0, t, rows, :])
            for e in range(EXP_DEV):
                xs[e, s * cap : (s + 1) * cap, cols] = got[e * cap : (e + 1) * cap].astype(BF)
                gs[e, s * cap : (s + 1) * cap, cols] = (
                    grad[e * cap : (e + 1) * cap] * slot_gates[s * EXP_DEV + e]
                ).astype(BF)
    for e in range(EXP_DEV):
        gate_col = jnp.concatenate([slot_gates[s * EXP_DEV + e] for s in range(seqs)], axis=0)
        both = matmul(xs[e], wgu[e])
        gated = both[:, :half]
        upper = both[:, half:]
        sig = jax.nn.sigmoid(gated)
        act = gated * sig
        hidden = (act * upper).astype(BF)
        grad_hidden = matmul_rows(gs[e], wd[e])
        grad_gu = jnp.concatenate(
            [
                (grad_hidden * upper * sig * (1.0 + gated * (1.0 - sig))).astype(BF),
                (grad_hidden * act).astype(BF),
            ],
            axis=1,
        )
        part = (matmul(hidden, wd[e]) * gate_col).astype(BF)
        back = matmul_rows(grad_gu, wgu[e]).astype(BF)
        for s in range(seqs):
            parts[s, e * cap : (e + 1) * cap, :] = part[s * cap : (s + 1) * cap]
            backs[s, e * cap : (e + 1) * cap, :] = back[s * cap : (s + 1) * cap]
        acc_d[e] += matmul_cols(hidden, gs[e])
        acc_gu[e] += matmul_cols(xs[e], grad_gu)
    for s in range(seqs):
        for t in range(tensors):
            cols = slice(t * width, (t + 1) * width)
            rows = slice(s * SEQ, (s + 1) * SEQ)
            out[0, t, 0, rows, :] = matmul_cols(picks[s], parts[s, :, cols]).astype(BF)
            out[0, t, 1, rows, :] = matmul_cols(picks[s], backs[s, :, cols]).astype(BF)

    @pl.when(step == pl.num_programs(0) - 1)
    def _():
        first = pltpu.make_async_copy(acc_gu, dgu, sems.at[0])
        second = pltpu.make_async_copy(acc_d, dd, sems.at[1])
        first.start()
        second.start()
        first.wait()
        second.wait()


def run_experts(slots, gates, x, og, wgu, wd, cap):
    groups, tensors, count, width = x.shape
    seqs = count // SEQ
    half = wd.shape[1]
    rows = slots.shape[1]
    stream = lambda g: (g, 0, 0, 0)
    return pl.pallas_call(
        functools.partial(expert_kernel, seqs, cap, tensors),
        grid=(groups,),
        in_specs=[
            pl.BlockSpec((1, rows, SEQ), lambda g: (g, 0, 0)),
            pl.BlockSpec((1, rows, SEQ), lambda g: (g, 0, 0)),
            pl.BlockSpec((1, tensors, count, width), stream),
            pl.BlockSpec((1, tensors, count, width), stream),
            pl.BlockSpec(wgu.shape, lambda g: (0, 0, 0), pipeline_mode=pl.Buffered(1)),
            pl.BlockSpec(wd.shape, lambda g: (0, 0, 0), pipeline_mode=pl.Buffered(1)),
        ],
        out_specs=[
            pl.BlockSpec((1, tensors, 2, count, width), lambda g: (g, 0, 0, 0, 0)),
            pl.BlockSpec(memory_space=pl.ANY),
            pl.BlockSpec(memory_space=pl.ANY),
        ],
        out_shape=[
            jax.ShapeDtypeStruct((groups, tensors, 2, count, width), BF),
            jax.ShapeDtypeStruct(wgu.shape, F32),
            jax.ShapeDtypeStruct(wd.shape, F32),
        ],
        scratch_shapes=[
            pltpu.VMEM((EXP_DEV, seqs * cap, D), BF),
            pltpu.VMEM((EXP_DEV, seqs * cap, D), BF),
            pltpu.VMEM((seqs, EXP_DEV * cap, D), BF),
            pltpu.VMEM((seqs, EXP_DEV * cap, D), BF),
            pltpu.VMEM(wgu.shape, F32),
            pltpu.VMEM(wd.shape, F32),
            pltpu.SemaphoreType.DMA((2,)),
        ],
        compiler_params=pltpu.CompilerParams(
            dimension_semantics=("arbitrary",), vmem_limit_bytes=60 * 1024 * 1024
        ),
        cost_estimate=pl.CostEstimate(
            flops=groups * EXP_DEV * seqs * cap * D * (half * 18 + SEQ * 8),
            bytes_accessed=groups * tensors * count * width * 8 + wgu.size * 9,
            transcendentals=groups * EXP_DEV * seqs * cap * half,
        ),
        name="experts",
    )(slots, gates, x, og, wgu, wd)


def local_wide(
    hidden_in,
    out_grad,
    first_gain,
    query_weight,
    latent_weight,
    latent_gain,
    expand_weight,
    output_weight,
    second_gain,
    shared_gate,
    shared_up,
    shared_down,
    expert_gate,
    expert_up,
    expert_down,
    routes,
    gate_values,
):
    groups = lax.axis_size("expert")
    tensors = lax.axis_size("tensor")
    place = lax.axis_index("tensor")
    mine = lax.axis_index("expert")
    experts_all = EXP_DEV * groups
    cap = SEQ * TOP * 4 // (3 * experts_all)
    width = D // tensors
    heads = H // tensors
    count = hidden_in.shape[0]
    seqs = count // SEQ
    rows_dev = D // groups
    scale = (DN + DR) ** (-0.5)
    cosine, sine = rope_tables(SEQ, DR)
    blocks = jnp.arange(SEQ, dtype=jnp.int32) // BLOCK
    allowed = (blocks[None, :] <= blocks[:, None])[None, None]

    whole_in = lax.all_gather(hidden_in, "tensor", axis=1, tiled=True)
    qc = query_weight.shape[1]
    oc = output_weight.shape[1]
    lc = latent_weight.shape[1]
    sc = shared_gate.shape[1]
    er, ec = expand_weight.shape
    cut = er * ec // rows_dev
    fold = rows_dev // er
    expand_rows = jnp.concatenate(
        [expand_weight[:, i * cut : (i + 1) * cut] for i in range(fold)], axis=0
    )
    attn_all = lax.all_gather(
        jnp.concatenate([query_weight, output_weight, expand_rows, latent_weight], axis=1),
        "expert",
        axis=0,
        tiled=True,
    )
    full_query = attn_all[:, :qc]
    full_output = attn_all[:, qc : qc + oc]
    full_latent = attn_all[:, qc + oc + cut :]
    full_expand = (
        attn_all[:, qc + oc : qc + oc + cut]
        .reshape(groups, fold, er, cut)
        .transpose(0, 2, 1, 3)
        .reshape(groups * er, ec)
    )
    gains = lax.all_gather(
        jnp.concatenate([first_gain, second_gain, latent_gain]).astype(F32), "expert", axis=0
    )
    gain_first = gains[:, :rows_dev].reshape(-1)
    gain_mid = gains[:, rows_dev : 2 * rows_dev].reshape(-1)
    gain_kv = gains[:, 2 * rows_dev :].reshape(-1)
    table = lax.all_gather(
        jnp.concatenate([routes.T.astype(F32), gate_values.T], axis=0), "expert", axis=0
    )
    pieces = max(1, min(seqs, groups // 8))
    per = count // pieces

    def to_all(rows):
        return lax.all_gather(rows, ("expert", "tensor"), axis=0).reshape(
            groups, tensors, per, width
        )

    og_first = to_all(out_grad[:per])
    shared_all = lax.all_gather(
        jnp.concatenate([shared_gate, shared_up, shared_down], axis=1), "expert", axis=0, tiled=True
    )
    full_sgu = shared_all[:, : 2 * sc]
    full_sdown = shared_all[:, 2 * sc :]

    inputs = whole_in.astype(F32)
    first_scale = rms_scale(inputs)
    first_hat = inputs * first_scale
    normed = (first_hat * gain_first).astype(BF)
    query = matmul(normed, full_query).reshape(seqs, SEQ, heads, DN + DR)
    latent = matmul(normed, full_latent)
    compressed = latent[:, :KV_RANK]
    latent_scale = rms_scale(compressed)
    latent_hat = compressed * latent_scale
    latent_normed = (latent_hat * gain_kv).astype(BF)
    expanded = matmul(latent_normed, full_expand).reshape(seqs, SEQ, heads, DN + DV)
    queries = jnp.concatenate(
        [query[..., :DN], rotate(query[..., DN:], cosine[:, None, :], sine[:, None, :])], axis=-1
    ).astype(BF)
    key_rope = rotate(latent[:, KV_RANK:].reshape(seqs, SEQ, DR), cosine, sine).astype(BF)
    keys = jnp.concatenate(
        [
            expanded[..., :DN].astype(BF),
            jnp.broadcast_to(key_rope[:, :, None, :], (seqs, SEQ, heads, DR)),
        ],
        axis=-1,
    )
    values = expanded[..., DN:].astype(BF)
    scores = jnp.where(
        allowed,
        jnp.einsum("nqhc,nkhc->nhqk", queries, keys, preferred_element_type=F32) * scale,
        masked_value,
    )
    peak = jnp.max(scores, axis=-1, keepdims=True)
    log_total = peak + jnp.log(jnp.sum(jnp.exp(scores - peak), axis=-1, keepdims=True))
    weights = jnp.exp(scores - log_total)
    mixed = (
        jnp.einsum("nhqk,nkhc->nqhc", weights.astype(BF), values, preferred_element_type=F32)
        .astype(BF)
        .reshape(count, heads * DV)
    )
    attended = lax.psum(matmul_rows(mixed, full_output).astype(BF), "tensor").astype(F32)
    middle = inputs + attended
    second_scale = rms_scale(middle)
    second_hat = middle * second_scale
    mixer_in = (second_hat * gain_mid).astype(BF)
    mixer_slice = lax.dynamic_slice_in_dim(mixer_in, place * width, width, 1)

    local_experts = (mine * EXP_DEV + jnp.arange(EXP_DEV, dtype=jnp.int32)).astype(F32)
    route_t = table[:, :TOP].reshape(groups, TOP, seqs, SEQ)
    gate_t = table[:, TOP:].reshape(groups, TOP, seqs, SEQ)
    named = route_t[:, :, :, None, :] == local_experts[None, None, None, :, None]
    gate_of = jnp.sum(jnp.where(named, gate_t[:, :, :, None, :], 0.0), axis=1)
    used = jnp.any(named, axis=1)
    before = (
        jnp.arange(SEQ, dtype=jnp.int32)[:, None] < jnp.arange(SEQ, dtype=jnp.int32)[None, :]
    ).astype(BF)
    prior = jnp.einsum("gset,tu->gseu", used.astype(BF), before, preferred_element_type=F32)
    slot_of = jnp.where(used & (prior < cap), prior, -1.0).astype(jnp.int32)
    slot_of = slot_of.reshape(groups, seqs * EXP_DEV, SEQ)
    gate_of = gate_of.reshape(groups, seqs * EXP_DEV, SEQ)

    ff = expert_gate.shape[2]
    half = -(-ff // 128) * 128
    wide = ((0, 0), (0, 0), (0, half - ff))
    wgu = jnp.concatenate([jnp.pad(expert_gate, wide), jnp.pad(expert_up, wide)], axis=2)
    wd = jnp.pad(expert_down, ((0, 0), (0, half - ff), (0, 0)))
    rows = slot_of.shape[1] // pieces
    sums = []
    dgu = dd = None
    for i in range(pieces):
        span = slice(i * per, (i + 1) * per)
        mixer_rows, og_rows = mixer_slice[span], out_grad[span]
        if i > 0:
            mixer_rows, og_rows, *sums = lax.optimization_barrier((mixer_rows, og_rows, *sums))
        outs, g_gu, g_d = run_experts(
            slot_of[:, i * rows : (i + 1) * rows],
            gate_of[:, i * rows : (i + 1) * rows],
            to_all(mixer_rows),
            og_first if i == 0 else to_all(og_rows),
            wgu,
            wd,
            cap,
        )
        dgu = g_gu if dgu is None else dgu + g_gu
        dd = g_d if dd is None else dd + g_d
        summed = lax.psum_scatter(
            outs.reshape(groups * tensors * 2 * per, width),
            ("expert", "tensor"),
            scatter_dimension=0,
            tiled=True,
        )
        sums.append(summed.reshape(2, per, width))
    summed = jnp.concatenate(sums, axis=1) if pieces > 1 else sums[0]
    total_gate = dgu[:, :, :ff]
    total_up = dgu[:, :, half : half + ff]
    total_down = dd[:, :ff]

    if pieces == 1:
        whole_grad = lax.dynamic_slice_in_dim(og_first, mine, 1, 0)[0]
        whole_grad = whole_grad.transpose(1, 0, 2).reshape(count, D)
    else:
        whole_grad = lax.all_gather(out_grad, "tensor", axis=1, tiled=True)
    shared_gu = matmul(mixer_in, full_sgu)
    shared_g = shared_gu[:, :sc]
    shared_u = shared_gu[:, sc:]
    shared_sig = jax.nn.sigmoid(shared_g)
    shared_hidden = (shared_g * shared_sig * shared_u).astype(BF)
    shared_part = matmul_rows(shared_hidden, full_sdown)
    grad_shared = matmul(whole_grad, full_sdown)
    step_sdown = matmul_cols(whole_grad, shared_hidden)
    grad_sg = (grad_shared * shared_u * shared_sig * (1.0 + shared_g * (1.0 - shared_sig))).astype(
        BF
    )
    grad_su = (grad_shared * shared_g * shared_sig).astype(BF)
    grad_sgu = jnp.concatenate([grad_sg, grad_su], axis=1)
    step_sgu = matmul_cols(mixer_in, grad_sgu)
    mixer_part = matmul_rows(grad_sgu, full_sgu)
    shared_sums = lax.psum_scatter(
        jnp.concatenate([shared_part.astype(BF), mixer_part.astype(BF)], axis=0),
        "tensor",
        scatter_dimension=1,
        tiled=True,
    )
    middle_slice = lax.dynamic_slice_in_dim(middle, place * width, width, 1)
    block_out = (
        middle_slice + summed[0].astype(F32) + shared_sums[:count].astype(F32)
    ).astype(BF)
    grad_mixer = lax.all_gather(
        (summed[1].astype(F32) + shared_sums[count:].astype(F32)).astype(BF),
        "tensor",
        axis=1,
        tiled=True,
    ).astype(F32)
    shared_steps = lax.psum_scatter(
        jnp.concatenate([step_sgu.astype(BF), step_sdown.astype(BF)], axis=1),
        "expert",
        scatter_dimension=0,
        tiled=True,
    ).astype(F32)

    step_gain_two = jnp.sum(grad_mixer * second_hat, axis=0)
    grad_middle = whole_grad.astype(F32) + norm_back(
        grad_mixer * gain_mid, second_hat, second_scale
    )
    grad_att = grad_middle.astype(BF)
    step_output = matmul_cols(grad_att, mixed)
    grad_mixed = matmul(grad_att, full_output).astype(BF).reshape(seqs, SEQ, heads, DV)
    grad_weights = jnp.einsum(
        "nqhc,nkhc->nhqk", grad_mixed, values, preferred_element_type=F32
    )
    grad_scores = (
        weights * (grad_weights - jnp.sum(weights * grad_weights, axis=-1, keepdims=True))
    ).astype(BF)
    grad_values = jnp.einsum(
        "nhqk,nqhc->nkhc", weights.astype(BF), grad_mixed, preferred_element_type=F32
    )
    grad_queries = (
        jnp.einsum("nhqk,nkhc->nqhc", grad_scores, keys, preferred_element_type=F32) * scale
    )
    grad_keys = (
        jnp.einsum("nhqk,nqhc->nkhc", grad_scores, queries, preferred_element_type=F32) * scale
    )
    grad_query = (
        jnp.concatenate(
            [
                grad_queries[..., :DN],
                unrotate(grad_queries[..., DN:], cosine[:, None, :], sine[:, None, :]),
            ],
            axis=-1,
        )
        .astype(BF)
        .reshape(count, heads * (DN + DR))
    )
    step_query = matmul_cols(normed, grad_query)
    query_part = matmul_rows(grad_query, full_query)
    rope_part = unrotate(jnp.sum(grad_keys[..., DN:], axis=2), cosine, sine).reshape(count, DR)
    grad_expanded = (
        jnp.concatenate([grad_keys[..., :DN], grad_values], axis=-1)
        .astype(BF)
        .reshape(count, heads * (DN + DV))
    )
    step_expand = matmul_cols(latent_normed, grad_expanded)
    latent_part = matmul_rows(grad_expanded, full_expand)
    latent_sum = lax.psum(
        jnp.concatenate([latent_part.astype(BF), rope_part.astype(BF)], axis=1), "tensor"
    ).astype(F32)
    grad_lnormed = latent_sum[:, :KV_RANK]
    step_gain_latent = jnp.sum(grad_lnormed * latent_hat, axis=0)
    grad_compressed = norm_back(grad_lnormed * gain_kv, latent_hat, latent_scale)
    grad_lat = jnp.concatenate([grad_compressed, latent_sum[:, KV_RANK:]], axis=-1).astype(BF)
    step_latent = matmul_cols(normed, grad_lat)
    query_sum = lax.psum_scatter(
        query_part.astype(BF), "tensor", scatter_dimension=1, tiled=True
    ).astype(F32)
    latent_slice = lax.dynamic_slice_in_dim(full_latent, place * width, width, 0)
    grad_normed = query_sum + matmul_rows(grad_lat, latent_slice)
    first_hat_slice = lax.dynamic_slice_in_dim(first_hat, place * width, width, 1)
    gain_first_slice = lax.dynamic_slice_in_dim(gain_first, place * width, width, 0)
    grad_hat = grad_normed * gain_first_slice
    row_dot = lax.psum(jnp.sum(grad_hat * first_hat_slice, axis=1), "tensor") / D
    grad_middle_slice = lax.dynamic_slice_in_dim(grad_middle, place * width, width, 1)
    input_grad = grad_middle_slice + first_scale * (grad_hat - first_hat_slice * row_dot[:, None])
    step_gain_one = jnp.sum(grad_normed * first_hat_slice, axis=0)

    expand_back = (
        step_expand.astype(BF)
        .reshape(groups, er, fold, cut)
        .transpose(0, 2, 1, 3)
        .reshape(groups * rows_dev, cut)
    )
    attn_steps = lax.psum_scatter(
        jnp.concatenate(
            [step_query.astype(BF), step_output.astype(BF), expand_back, step_latent.astype(BF)],
            axis=1,
        ),
        "expert",
        scatter_dimension=0,
        tiled=True,
    ).astype(F32)
    grad_expand = attn_steps[:, qc + oc : qc + oc + cut]
    grad_expand = jnp.concatenate(
        [grad_expand[i * er : (i + 1) * er] for i in range(fold)], axis=1
    )
    one_full = lax.dynamic_update_slice_in_dim(
        jnp.zeros((D,), F32), step_gain_one, place * width, 0
    )
    gain_sums = lax.psum(
        jnp.concatenate([one_full, step_gain_two / tensors, step_gain_latent / tensors]),
        ("expert", "tensor"),
    )
    kv_dev = latent_gain.shape[0]
    return (
        block_out,
        input_grad,
        lax.dynamic_slice_in_dim(gain_sums, mine * rows_dev, rows_dev, 0),
        attn_steps[:, :qc],
        attn_steps[:, qc + oc + cut :],
        lax.dynamic_slice_in_dim(gain_sums, 2 * D + mine * kv_dev, kv_dev, 0),
        grad_expand,
        attn_steps[:, qc : qc + oc],
        lax.dynamic_slice_in_dim(gain_sums, D + mine * rows_dev, rows_dev, 0),
        shared_steps[:, :sc],
        shared_steps[:, sc : 2 * sc],
        shared_steps[:, 2 * sc :],
        total_gate,
        total_up,
        total_down,
    )


MESH = pl.DeviceIdType.MESH


def mixer_kernel(
    cap,
    slots, gates, mx_in, og_all, wgu, wd, shared,
    back_sum, routed, d_shared, o_xs, o_gs, o_gu, o_hid, mxb, mxp, cb,
    wgu_v, wd_v, shared_v, full_x, full_og, xs, gs, gu_b, hid_b, parts, backs, hid_s, gu_s,
    rstage, keep0, keep2, send, cstage, ysend, yb, xb, zsend, zb,
    az_s, az_r, ax_s, ax_r, ac_s, ac_r, rc_s, rc_r, ry_s, ry_r, rx_s, rx_r, rz_s, rz_r,
    w_sem, in_sem, og_sem, save_sem, rout_sem, cst_sem,
):
    groups, tensors, count, width = og_all.shape
    ring = groups // 2
    seqs = count // SEQ
    half = wd.shape[1]
    units = shared.shape[0] // 3
    chunks = D // width
    mine = lax.axis_index("expert")
    place_t = lax.axis_index("tensor")
    z = lax.div(mine, 2)
    x = lax.rem(mine, 2)
    y = lax.div(place_t, 2)
    c = lax.rem(place_t, 2)
    at_x = (z * 2 + 1 - x, place_t)
    at_y = (mine, (1 - y) * 2 + c)
    at_c = (mine, y * 2 + 1 - c)
    at_z = (lax.rem(z + 1, ring) * 2 + x, place_t)
    from_z = (lax.rem(z + ring - 1, ring) * 2 + x, place_t)

    def remote(src, dst, s_sem, r_sem, to):
        return pltpu.make_async_remote_copy(
            src_ref=src, dst_ref=dst, send_sem=s_sem, recv_sem=r_sem, device_id=to, device_id_type=MESH
        )

    def place_of(rel):
        return lax.rem(y + rel // 2, 2) * 2 + lax.rem(c + rel % 2, 2)

    def cols_of(rel):
        return pl.ds(pl.multiple_of(place_of(rel) * width, width), width)

    def group_of(i):
        k = lax.div(i, 2)
        return lax.rem(z + ring - k, ring) * 2 + lax.rem(x + lax.rem(i, 2), 2)

    loads = [
        pltpu.make_async_copy(shared, shared_v, w_sem.at[0]),
        pltpu.make_async_copy(wgu, wgu_v, w_sem.at[1]),
        pltpu.make_async_copy(wd, wd_v, w_sem.at[2]),
    ]
    for load in loads:
        load.start()

    def og_copies(i, slot):
        g = group_of(i)
        return [
            pltpu.make_async_copy(
                og_all.at[g, t],
                full_og.at[slot, :, pl.ds(t * width, width)],
                og_sem.at[slot, t],
            )
            for t in range(tensors)
        ]

    for copy in og_copies(0, 0):
        copy.start()

    barrier = pltpu.get_barrier_semaphore()
    for to in (at_x, at_y, at_c, at_z, from_z):
        pl.semaphore_signal(barrier, inc=1, device_id=to, device_id_type=MESH)
    pl.semaphore_wait(barrier, 5)

    def z_hop(k, src):
        return remote(src, mxb.at[2 * k + 2], az_s.at[k], az_r.at[k], at_z)

    def x_hop(k, src):
        return remote(src, mxb.at[2 * k + 1], ax_s.at[k], ax_r.at[k], at_x)

    def c_hop(i, src):
        return remote(src, mxp.at[i], ac_s.at[i], ac_r.at[i], at_c)

    z_hop(0, mx_in).start()
    x_hop(0, mx_in).start()
    c_hop(0, mx_in).start()
    d_shared[...] = jnp.zeros_like(d_shared)
    loads[0].wait()

    iota = lax.broadcasted_iota(jnp.int32, (cap, SEQ), 0)

    def save_copies(i):
        return [
            pltpu.make_async_copy(xs, o_xs.at[:, i], save_sem.at[0]),
            pltpu.make_async_copy(gs, o_gs.at[:, i], save_sem.at[1]),
            pltpu.make_async_copy(gu_b, o_gu.at[:, i], save_sem.at[2]),
            pltpu.make_async_copy(hid_b, o_hid.at[:, i], save_sem.at[3]),
        ]

    def rout_copies(i):
        g = group_of(i)
        return [
            pltpu.make_async_copy(rstage.at[rel], routed.at[g, place_of(rel)], rout_sem.at[rel])
            for rel in range(4)
        ]

    def c_back(i):
        return remote(send.at[lax.rem(i, 2)], cb.at[i], rc_s.at[i], rc_r.at[i], at_c)

    def y_back(i):
        return remote(ysend.at[lax.rem(i, 2)], yb.at[i], ry_s.at[i], ry_r.at[i], at_y)

    def x_back(k):
        return remote(keep0.at[2 * k + 1], xb.at[k], rx_s.at[k], rx_r.at[k], at_x)

    def z_back(n):
        return remote(zsend.at[n], zb.at[n], rz_s.at[n], rz_r.at[n], at_z)

    def compute(i):
        slot = lax.rem(i, 2)
        g = group_of(i)

        @pl.when(i + 1 < groups)
        def _():
            for copy in og_copies(i + 1, 1 - slot):
                copy.start()

        peer = [
            pltpu.make_async_copy(mxp.at[i, n], full_x.at[:, cols_of(2 * n + 1)], in_sem.at[2 + n])
            for n in range(2)
        ]

        @pl.when(i == 0)
        def _():
            own = [
                pltpu.make_async_copy(mx_in.at[n], full_x.at[:, cols_of(2 * n)], in_sem.at[n])
                for n in range(2)
            ]
            for copy in own:
                copy.start()
            for copy in own:
                copy.wait()

        @pl.when(i > 0)
        def _():
            own = [
                pltpu.make_async_copy(mxb.at[i, n], full_x.at[:, cols_of(2 * n)], in_sem.at[n])
                for n in range(2)
            ]
            for copy in own:
                copy.start()
            for copy in own:
                copy.wait()

        for copy in peer:
            copy.start()
        for copy in peer:
            copy.wait()
        for copy in og_copies(i, slot):
            copy.wait()

        @pl.when(i > 0)
        def _():
            for copy in save_copies(i - 1):
                copy.wait()

        picks = []
        gate_cols = []
        for s in range(seqs):
            chosen = []
            for e in range(EXP_DEV):
                row = s * EXP_DEV + e
                hit = iota == slots[g, row : row + 1, :]
                gate_cols.append(
                    jnp.sum(jnp.where(hit, gates[g, row : row + 1, :], 0.0), axis=1, keepdims=True)
                )
                chosen.append(hit.astype(F32).astype(BF))
            picks.append(jnp.concatenate(chosen, axis=0))
        for s in range(seqs):
            rows = slice(s * SEQ, (s + 1) * SEQ)
            here = slice(s * cap, (s + 1) * cap)
            for n in range(chunks):
                cols = slice(n * width, (n + 1) * width)
                got = matmul(picks[s], full_x[rows, cols])
                grad = matmul(picks[s], full_og[slot, rows, cols])
                for e in range(EXP_DEV):
                    xs[e, here, cols] = got[e * cap : (e + 1) * cap].astype(BF)
                    gs[e, here, cols] = (
                        grad[e * cap : (e + 1) * cap] * gate_cols[s * EXP_DEV + e]
                    ).astype(BF)
        both = matmul_rows(full_x[...], shared_v[: 2 * units])
        gated = both[:, :units]
        upper = both[:, units:]
        sig = jax.nn.sigmoid(gated)
        act = gated * sig
        grad = matmul_rows(full_og[slot], shared_v[2 * units :])
        hid_s[...] = (act * upper).astype(BF)
        gu_s[:, :units] = (grad * upper * sig * (1.0 + gated * (1.0 - sig))).astype(BF)
        gu_s[:, units:] = (grad * act).astype(BF)
        for n in range(chunks):
            cols = slice(n * width, (n + 1) * width)
            d_shared[: 2 * units, cols] += matmul_cols(gu_s[...], full_x[:, cols])
            d_shared[2 * units :, cols] += matmul_cols(hid_s[...], full_og[slot, :, cols])

        @pl.when(i == 0)
        def _():
            loads[1].wait()
            loads[2].wait()

        for e in range(EXP_DEV):
            gate_col = jnp.concatenate([gate_cols[s * EXP_DEV + e] for s in range(seqs)], axis=0)
            both = matmul(xs[e], wgu_v[e])
            gated = both[:, :half]
            upper = both[:, half:]
            sig = jax.nn.sigmoid(gated)
            act = gated * sig
            hid_b[e] = (act * upper).astype(BF)
            grad = matmul_rows(gs[e], wd_v[e])
            gu_b[e, :, :half] = (grad * upper * sig * (1.0 + gated * (1.0 - sig))).astype(BF)
            gu_b[e, :, half:] = (grad * act).astype(BF)
            for n in range(chunks):
                cols = slice(n * width, (n + 1) * width)
                part = (matmul(hid_b[e], wd_v[e, :, cols]) * gate_col).astype(BF)
                back = matmul_rows(gu_b[e], wgu_v[e, cols, :]).astype(BF)
                for s in range(seqs):
                    there = slice(e * cap, (e + 1) * cap)
                    parts[s, there, cols] = part[s * cap : (s + 1) * cap]
                    backs[s, there, cols] = back[s * cap : (s + 1) * cap]
        for copy in save_copies(i):
            copy.start()

        @pl.when(i >= 2)
        def _():
            c_back(i - 2).wait_send()

        @pl.when(i >= 1)
        def _():
            for copy in rout_copies(i - 1):
                copy.wait()

        for rel in (1, 3, 0, 2):
            cols = cols_of(rel)
            for s in range(seqs):
                rows = slice(s * SEQ, (s + 1) * SEQ)
                back = (
                    matmul_cols(picks[s], backs[s, :, cols])
                    + matmul(gu_s[rows, :], shared_v[: 2 * units, cols])
                ).astype(BF)
                if rel == 0:
                    keep0[i, rows, :] = back
                elif rel == 2:
                    keep2[slot, rows, :] = back
                else:
                    send[slot, rel // 2, rows, :] = back
            if rel == 3:
                c_back(i).start()
        for rel in range(4):
            cols = cols_of(rel)
            for s in range(seqs):
                rows = slice(s * SEQ, (s + 1) * SEQ)
                rstage[rel, rows, :] = (
                    matmul_cols(picks[s], parts[s, :, cols])
                    + matmul(hid_s[rows, :], shared_v[2 * units :, cols])
                ).astype(BF)
        for copy in rout_copies(i):
            copy.start()

    def step(i, carry):
        k = lax.div(i, 2)
        odd = lax.rem(i, 2) == 1

        @pl.when(jnp.logical_and(odd, i < groups))
        def _():
            x_hop(k, mxb.at[2 * k]).wait_recv()
            c_hop(i, mxb.at[i]).start()

        @pl.when(jnp.logical_and(odd, i < groups - 1))
        def _():
            z_hop(k, mxb.at[2 * k]).wait_recv()

            @pl.when(k + 2 < ring)
            def _():
                z_hop(k + 1, mxb.at[2 * k + 2]).start()

            x_hop(k + 1, mxb.at[2 * k + 2]).start()
            c_hop(i + 1, mxb.at[i + 1]).start()

        @pl.when(i < groups)
        def _():
            c_hop(i, mxb.at[i]).wait_recv()
            compute(i)

        @pl.when(jnp.logical_and(i >= 1, i < groups + 1))
        def _():
            j = i - 1
            c_back(j).wait_recv()
            fetch = pltpu.make_async_copy(cb.at[j], cstage, cst_sem)
            fetch.start()

            @pl.when(j >= 2)
            def _():
                y_back(j - 2).wait_send()

            fetch.wait()
            ysend[lax.rem(j, 2)] = (
                keep2[lax.rem(j, 2)].astype(F32) + cstage[1].astype(F32)
            ).astype(BF)
            y_back(j).start()
            keep0[j] = (keep0[j].astype(F32) + cstage[0].astype(F32)).astype(BF)

        @pl.when(jnp.logical_and(i >= 3, i < groups + 3))
        def _():
            j = i - 3
            y_back(j).wait_recv()
            keep0[j] = (keep0[j].astype(F32) + yb[j].astype(F32)).astype(BF)

            @pl.when(lax.rem(j, 2) == 1)
            def _():
                x_back(lax.div(j, 2)).start()

        for p in range(ring):

            @pl.when(i == 2 * p + 6)
            def _():
                x_back(p).wait_recv()
                total = keep0[2 * p].astype(F32) + xb[p].astype(F32)
                if p == 0:
                    keep0[0] = total.astype(BF)
                elif p == 1:
                    zsend[0] = total.astype(BF)
                    z_back(0).start()
                else:
                    z_back(p - 2).wait_recv()
                    zsend[p - 1] = (total + zb[p - 2].astype(F32)).astype(BF)
                    z_back(p - 1).start()

        return carry

    lax.fori_loop(0, groups + 5, step, 0)
    z_back(ring - 2).wait_recv()
    back_sum[...] = (keep0[0].astype(F32) + zb[ring - 2].astype(F32)).astype(BF)
    for copy in save_copies(groups - 1):
        copy.wait()
    for copy in rout_copies(groups - 1):
        copy.wait()
    for n in range(ring - 1):
        z_hop(n, mx_in).wait_send()
        z_back(n).wait_send()
    for n in range(ring):
        x_hop(n, mx_in).wait_send()
        x_back(n).wait_send()
    for n in range(groups):
        c_hop(n, mx_in).wait_send()
    for n in (groups - 2, groups - 1):
        c_back(n).wait_send()
        y_back(n).wait_send()


def run_mixer(cap, slots, gates, mx, og_all, wgu, wd, shared):
    groups, tensors, count, width = og_all.shape
    seqs = count // SEQ
    half = wd.shape[1]
    units = shared.shape[0] // 3
    ring = groups // 2
    rows = seqs * cap
    hbm = pl.BlockSpec(memory_space=pl.ANY)
    vmem = pl.BlockSpec(memory_space=pltpu.VMEM)
    block = (count, width)
    dma = pltpu.SemaphoreType.DMA
    out = lambda shape, dtype=BF: jax.ShapeDtypeStruct(shape, dtype)
    return pl.pallas_call(
        functools.partial(mixer_kernel, cap),
        in_specs=[vmem, vmem, hbm, hbm, hbm, hbm, hbm],
        out_specs=[vmem, hbm, vmem, hbm, hbm, hbm, hbm, hbm, hbm, hbm],
        out_shape=[
            out(block),
            out(og_all.shape),
            out((3 * units, D), F32),
            out((EXP_DEV, groups, rows, D)),
            out((EXP_DEV, groups, rows, D)),
            out((EXP_DEV, groups, rows, 2 * half)),
            out((EXP_DEV, groups, rows, half)),
            out((groups, 2, *block)),
            out((groups, 2, *block)),
            out((groups, 2, *block)),
        ],
        scratch_shapes=[
            pltpu.VMEM(wgu.shape, BF),
            pltpu.VMEM(wd.shape, BF),
            pltpu.VMEM(shared.shape, BF),
            pltpu.VMEM((count, D), BF),
            pltpu.VMEM((2, count, D), BF),
            pltpu.VMEM((EXP_DEV, rows, D), BF),
            pltpu.VMEM((EXP_DEV, rows, D), BF),
            pltpu.VMEM((EXP_DEV, rows, 2 * half), BF),
            pltpu.VMEM((EXP_DEV, rows, half), BF),
            pltpu.VMEM((seqs, EXP_DEV * cap, D), BF),
            pltpu.VMEM((seqs, EXP_DEV * cap, D), BF),
            pltpu.VMEM((count, units), BF),
            pltpu.VMEM((count, 2 * units), BF),
            pltpu.VMEM((4, *block), BF),
            pltpu.VMEM((groups, *block), BF),
            pltpu.VMEM((2, *block), BF),
            pltpu.VMEM((2, 2, *block), BF),
            pltpu.VMEM((2, *block), BF),
            pltpu.VMEM((2, *block), BF),
            pltpu.VMEM((groups, *block), BF),
            pltpu.VMEM((ring, *block), BF),
            pltpu.VMEM((ring - 1, *block), BF),
            pltpu.VMEM((ring - 1, *block), BF),
            dma((ring - 1,)), dma((ring - 1,)), dma((ring,)), dma((ring,)), dma((groups,)), dma((groups,)),
            dma((groups,)), dma((groups,)), dma((groups,)), dma((groups,)), dma((ring,)), dma((ring,)),
            dma((ring - 1,)), dma((ring - 1,)),
            dma((3,)), dma((4,)), dma((2, tensors)), dma((4,)), dma((4,)), dma,
        ],
        compiler_params=pltpu.CompilerParams(
            collective_id=1, has_side_effects=True, vmem_limit_bytes=60 * 1024 * 1024
        ),
        cost_estimate=pl.CostEstimate(
            flops=80_000_000_000,
            bytes_accessed=200 * 1024 * 1024,
            transcendentals=8_000_000,
        ),
        name="mixer",
    )(slots, gates, mx, og_all, wgu, wd, shared)


def weight_kernel(xs, gs, gu, hid, d_gate, d_up, d_down, acc_gu, acc_d):
    g = pl.program_id(1)
    ff = d_gate.shape[-1]
    half = hid.shape[-1]

    @pl.when(g == 0)
    def _():
        acc_gu[...] = jnp.zeros_like(acc_gu)
        acc_d[...] = jnp.zeros_like(acc_d)

    for i in range(xs.shape[1]):
        acc_gu[...] += matmul_cols(xs[0, i], gu[0, i])
        acc_d[...] += matmul_cols(hid[0, i], gs[0, i])

    @pl.when(g == pl.num_programs(1) - 1)
    def _():
        d_gate[0] = acc_gu[:, :ff]
        d_up[0] = acc_gu[:, half : half + ff]
        d_down[0] = acc_d[:ff]


def weight_grads(xs, gs, gu, hid, ff):
    groups, rows = xs.shape[1:3]
    half = hid.shape[-1]
    step = 2
    slab = lambda last: pl.BlockSpec((1, step, rows, last), lambda e, g: (e, g, 0, 0))
    out = lambda *dims: pl.BlockSpec((1, *dims), lambda e, g: (e, 0, 0))
    return pl.pallas_call(
        weight_kernel,
        grid=(EXP_DEV, groups // step),
        in_specs=[slab(D), slab(D), slab(2 * half), slab(half)],
        out_specs=[out(D, ff), out(D, ff), out(ff, D)],
        out_shape=[
            jax.ShapeDtypeStruct((EXP_DEV, D, ff), F32),
            jax.ShapeDtypeStruct((EXP_DEV, D, ff), F32),
            jax.ShapeDtypeStruct((EXP_DEV, ff, D), F32),
        ],
        scratch_shapes=[pltpu.VMEM((D, 2 * half), F32), pltpu.VMEM((half, D), F32)],
        compiler_params=pltpu.CompilerParams(
            dimension_semantics=("arbitrary", "arbitrary"), vmem_limit_bytes=60 * 1024 * 1024
        ),
        cost_estimate=pl.CostEstimate(
            flops=EXP_DEV * groups * rows * D * half * 6,
            bytes_accessed=64 * 1024 * 1024,
            transcendentals=0,
        ),
        name="weight_grads",
    )(xs, gs, gu, hid)


def place_kernel(targets, n, *refs):
    blocks, out, sems = refs[:n], refs[n], refs[n + 1]
    copies = [
        pltpu.make_async_copy(block, out.at[target()], sems.at[i])
        for i, (block, target) in enumerate(zip(blocks, targets))
    ]
    for copy in copies:
        copy.start()
    for copy in copies:
        copy.wait()


def place(blocks, targets, count):
    n = len(blocks)
    return pl.pallas_call(
        functools.partial(place_kernel, targets, n),
        in_specs=[pl.BlockSpec(memory_space=pltpu.VMEM)] * n,
        out_specs=pl.BlockSpec(memory_space=pl.ANY),
        out_shape=jax.ShapeDtypeStruct((count, *blocks[0].shape), blocks[0].dtype),
        scratch_shapes=[pltpu.SemaphoreType.DMA((n,))],
        compiler_params=pltpu.CompilerParams(vmem_limit_bytes=16 * 1024 * 1024),
        name="place",
    )(*blocks)


def flip_tensor(x, mask):
    size = lax.axis_size("tensor")
    return lax.ppermute(x, "tensor", [(i, i ^ mask) for i in range(size)])


def to_core(x):
    return flip_tensor(x, 1)


def to_y(x):
    return flip_tensor(x, 2)


def to_x(x):
    size = lax.axis_size("expert")
    return lax.ppermute(x, "expert", [(i, i ^ 1) for i in range(size)])


def to_z(x):
    size = lax.axis_size("expert")
    return lax.ppermute(x, "expert", [(i, (i + 2) % size) for i in range(size)])


def after(x, done):
    return lax.optimization_barrier((x, done))[0]


def add(*terms):
    total = terms[0].astype(F32)
    for term in terms[1:]:
        total = total + term.astype(F32)
    return total.astype(BF)


def gather_pairs(block):
    ring = lax.axis_size("expert") // 2
    pairs = []
    for k in range(ring):
        pairs.append((block, to_x(block)))
        if k < ring - 1:
            block = to_z(block)
    return pairs


def group_at(k, xr):
    def target():
        mine = lax.axis_index("expert")
        ring = lax.axis_size("expert") // 2
        return lax.rem(mine // 2 + ring - k, ring) * 2 + jnp.bitwise_xor(lax.rem(mine, 2), xr)

    return target


def gather_rows(block):
    groups = lax.axis_size("expert")
    pairs = gather_pairs(block)
    blocks = [b for pair in pairs for b in pair]
    targets = [group_at(k, xr) for k in range(groups // 2) for xr in range(2)]
    return place(blocks, targets, groups)


def ring_sum(totals):
    ring = len(totals)
    moving = totals[1]()
    for k in range(2, ring):
        moving = add(to_z(moving), totals[k]())
    return to_z(moving), totals[0]()


def scatter_rows(blocks):
    ring = lax.axis_size("expert") // 2
    at = lambda k, xr: lax.dynamic_index_in_dim(blocks, group_at(k, xr)(), 0, keepdims=False)
    came = {}
    last = None
    for k in [*range(1, ring), 0]:
        sent = at(k, 1)
        if last is not None:
            sent = after(sent, last)
        last = to_x(sent)
        came[k] = last
    return ring_sum([lambda k=k: add(at(k, 0), came[k]) for k in range(ring)])


def pieces_of(x):
    other = to_y(x)
    return x, other, to_core(x), to_core(other)


def join(pieces, axis):
    place_t = lax.axis_index("tensor")
    low_y = place_t // 2 == 0
    low_c = lax.rem(place_t, 2) == 0
    o0, o2, o1, o3 = pieces
    a = (jnp.where(low_y, o0, o2), jnp.where(low_y, o2, o0))
    b = (jnp.where(low_y, o1, o3), jnp.where(low_y, o3, o1))
    out = []
    for y in range(2):
        out += [jnp.where(low_c, a[y], b[y]), jnp.where(low_c, b[y], a[y])]
    return jnp.concatenate(out, axis=axis)


def scatter_cols(x):
    place_t = lax.axis_index("tensor")
    rows = x.shape[0]
    view = x.reshape(rows, 2, 2, -1)
    low_y = place_t // 2 == 0
    low_c = lax.rem(place_t, 2) == 0
    keep = jnp.where(low_c, view[:, :, 0], view[:, :, 1])
    send = jnp.where(low_c, view[:, :, 1], view[:, :, 0])
    half = add(keep, to_core(send))
    mine = jnp.where(low_y, half[:, 0], half[:, 1])
    theirs = jnp.where(low_y, half[:, 1], half[:, 0])
    return mine, to_y(theirs)


def sum_cols(x):
    place_t = lax.axis_index("tensor")
    rows = x.shape[0]
    view = x.reshape(rows, 2, 2, -1)
    low_c = lax.rem(place_t, 2) == 0
    keep = jnp.where(low_c, view[:, :, 0], view[:, :, 1])
    send = jnp.where(low_c, view[:, :, 1], view[:, :, 0])
    half = add(keep, to_core(send))
    half = add(half, to_y(half))
    other = to_core(half)
    return jnp.stack(
        [jnp.where(low_c, half, other), jnp.where(low_c, other, half)], axis=2
    ).reshape(rows, -1)


def small_sum(x):
    x = x + to_core(x)
    return x + to_y(x)


def local(
    hidden_in,
    out_grad,
    first_gain,
    query_weight,
    latent_weight,
    latent_gain,
    expand_weight,
    output_weight,
    second_gain,
    shared_gate,
    shared_up,
    shared_down,
    expert_gate,
    expert_up,
    expert_down,
    routes,
    gate_values,
):
    groups = lax.axis_size("expert")
    tensors = lax.axis_size("tensor")
    ring = groups // 2
    place_t = lax.axis_index("tensor")
    mine = lax.axis_index("expert")
    experts_all = EXP_DEV * groups
    cap = SEQ * TOP * 4 // (3 * experts_all)
    width = D // tensors
    heads = H // tensors
    count = hidden_in.shape[0]
    seqs = count // SEQ
    rows_dev = D // groups
    scale = (DN + DR) ** (-0.5)
    cosine, sine = rope_tables(SEQ, DR)
    blocks = jnp.arange(SEQ, dtype=jnp.int32) // BLOCK
    allowed = (blocks[None, :] <= blocks[:, None])[None, None]
    qc = query_weight.shape[1]
    oc = output_weight.shape[1]
    lc = latent_weight.shape[1]
    sc = shared_gate.shape[1]
    er, ec = expand_weight.shape
    kv_dev = latent_gain.shape[0]
    cut = er * ec // rows_dev
    fold = rows_dev // er
    quarter = rows_dev // tensors

    gain_row = jnp.concatenate([first_gain, second_gain, latent_gain]).reshape(1, -1)
    lat_rows = lax.dynamic_slice_in_dim(latent_weight, place_t * quarter, quarter, 0)
    lat_all = gather_rows(jnp.concatenate([lat_rows, gain_row], axis=0))
    gains = lat_all[:, quarter].astype(F32)
    gain_first = gains[:, :rows_dev].reshape(-1)
    gain_mid = gains[:, rows_dev : 2 * rows_dev].reshape(-1)
    gain_kv = gains[:, 2 * rows_dev :].reshape(-1)
    full_latent = join(pieces_of(lat_all[:, :quarter]), 1).reshape(D, lc)
    expand_rows = jnp.concatenate(
        [expand_weight[:, i * cut : (i + 1) * cut] for i in range(fold)], axis=0
    )
    qe_all = gather_rows(jnp.concatenate([query_weight, output_weight, expand_rows], axis=1))
    full_query = qe_all[:, :, :qc].reshape(D, qc)
    full_expand = (
        qe_all[:, :, qc + oc :].reshape(groups, fold, er, cut).transpose(0, 2, 1, 3).reshape(groups * er, ec)
    )
    full_output = qe_all[:, :, qc : qc + oc].reshape(D, oc)

    units = sc // groups
    wide_units = -(-units // 128) * 128
    shared_t = jnp.stack([shared_gate.T, shared_up.T, shared_down.T]).reshape(3, groups, units, rows_dev)
    shared_t = shared_t.transpose(1, 0, 2, 3).reshape(groups, 3 * units, rows_dev)
    shared_t = lax.all_to_all(shared_t, "expert", split_axis=0, concat_axis=0, tiled=True)
    shared_t = shared_t.reshape(groups, 3, units, rows_dev).transpose(1, 2, 0, 3).reshape(3, units, D)
    shared_w = jnp.pad(shared_t, ((0, 0), (0, wide_units - units), (0, 0))).reshape(3 * wide_units, D)

    table = gather_rows(jnp.concatenate([routes.T.astype(F32), gate_values.T], axis=0))
    og_all = lax.all_gather(out_grad, ("expert", "tensor"), axis=0)
    og_all = og_all.reshape(groups, tensors, count, width)
    whole_grad = lax.dynamic_index_in_dim(og_all, mine, 0, keepdims=False)
    whole_grad = whole_grad.transpose(1, 0, 2).reshape(count, D)

    whole_in = join(pieces_of(hidden_in), 1)
    inputs = whole_in.astype(F32)
    first_scale = rms_scale(inputs)
    first_hat = inputs * first_scale
    normed = (first_hat * gain_first).astype(BF)
    query = matmul(normed, full_query).reshape(seqs, SEQ, heads, DN + DR)
    latent = matmul(normed, full_latent)
    compressed = latent[:, :KV_RANK]
    latent_scale = rms_scale(compressed)
    latent_hat = compressed * latent_scale
    latent_normed = (latent_hat * gain_kv).astype(BF)
    expanded = matmul(latent_normed, full_expand).reshape(seqs, SEQ, heads, DN + DV)
    queries = jnp.concatenate(
        [query[..., :DN], rotate(query[..., DN:], cosine[:, None, :], sine[:, None, :])], axis=-1
    ).astype(BF)
    key_rope = rotate(latent[:, KV_RANK:].reshape(seqs, SEQ, DR), cosine, sine).astype(BF)
    keys = jnp.concatenate(
        [
            expanded[..., :DN].astype(BF),
            jnp.broadcast_to(key_rope[:, :, None, :], (seqs, SEQ, heads, DR)),
        ],
        axis=-1,
    )
    values = expanded[..., DN:].astype(BF)
    scores = jnp.where(
        allowed,
        jnp.einsum("nqhc,nkhc->nhqk", queries, keys, preferred_element_type=F32) * scale,
        masked_value,
    )
    peak = jnp.max(scores, axis=-1, keepdims=True)
    log_total = peak + jnp.log(jnp.sum(jnp.exp(scores - peak), axis=-1, keepdims=True))
    weights = jnp.exp(scores - log_total)
    mixed = (
        jnp.einsum("nhqk,nkhc->nqhc", weights.astype(BF), values, preferred_element_type=F32)
        .astype(BF)
        .reshape(count, heads * DV)
    )
    attended = sum_cols(matmul_rows(mixed, full_output).astype(BF)).astype(F32)
    middle = inputs + attended
    second_scale = rms_scale(middle)
    second_hat = middle * second_scale
    mixer_in = (second_hat * gain_mid).astype(BF)
    low_y = place_t // 2 == 0
    low_c = lax.rem(place_t, 2) == 0
    view = mixer_in.reshape(count, 2, 2, width)
    view = jnp.where(low_c, view[:, :, 0], view[:, :, 1])
    mixer_half = jnp.stack(
        [jnp.where(low_y, view[:, 0], view[:, 1]), jnp.where(low_y, view[:, 1], view[:, 0])]
    )

    local_experts = (mine * EXP_DEV + jnp.arange(EXP_DEV, dtype=jnp.int32)).astype(F32)
    route_t = table[:, :TOP].reshape(groups, TOP, seqs, SEQ)
    gate_t = table[:, TOP:].reshape(groups, TOP, seqs, SEQ)
    named = route_t[:, :, :, None, :] == local_experts[None, None, None, :, None]
    gate_of = jnp.sum(jnp.where(named, gate_t[:, :, :, None, :], 0.0), axis=1)
    used = jnp.any(named, axis=1)
    before = (
        jnp.arange(SEQ, dtype=jnp.int32)[:, None] < jnp.arange(SEQ, dtype=jnp.int32)[None, :]
    ).astype(BF)
    prior = jnp.einsum("gset,tu->gseu", used.astype(BF), before, preferred_element_type=F32)
    slot_of = jnp.where(used & (prior < cap), prior, -1.0).astype(jnp.int32)
    slot_of = slot_of.reshape(groups, seqs * EXP_DEV, SEQ)
    gate_of = gate_of.reshape(groups, seqs * EXP_DEV, SEQ)

    ff = expert_gate.shape[2]
    half = -(-ff // 128) * 128
    wide = ((0, 0), (0, 0), (0, half - ff))
    wgu = jnp.concatenate([jnp.pad(expert_gate, wide), jnp.pad(expert_up, wide)], axis=2)
    wd = jnp.pad(expert_down, ((0, 0), (0, half - ff), (0, 0)))
    back_sum, rout, shared_step, *saved = run_mixer(
        cap, slot_of, gate_of, mixer_half, og_all, wgu, wd, shared_w
    )
    saved = saved[:4]
    rout_sum = lax.psum_scatter(
        rout.reshape(groups * tensors * count, width),
        ("expert", "tensor"),
        scatter_dimension=0,
        tiled=True,
    )
    total_gate, total_up, total_down = weight_grads(*saved, ff)
    middle_slice = lax.dynamic_slice_in_dim(middle, place_t * width, width, 1)
    block_out = (middle_slice + rout_sum.astype(F32)).astype(BF)
    shared_step = shared_step.reshape(3, wide_units, groups, rows_dev)[:, :units].astype(BF)
    shared_step = shared_step.transpose(2, 0, 1, 3).reshape(groups, 3 * units, rows_dev)
    shared_step = lax.all_to_all(shared_step, "expert", split_axis=0, concat_axis=0, tiled=True)
    shared_step = shared_step.reshape(groups, 3, units, rows_dev).transpose(1, 3, 0, 2)
    shared_step = shared_step.reshape(3, rows_dev, sc).astype(F32)

    grad_mixer = join(pieces_of(back_sum), 1).astype(F32)
    step_gain_two = jnp.sum(grad_mixer * second_hat, axis=0)
    grad_middle = whole_grad.astype(F32) + norm_back(
        grad_mixer * gain_mid, second_hat, second_scale
    )
    grad_att = grad_middle.astype(BF)
    step_output = matmul_cols(grad_att, mixed)
    output_sum = scatter_rows(step_output.astype(BF).reshape(groups, rows_dev, -1))
    grad_mixed = matmul(grad_att, full_output).astype(BF).reshape(seqs, SEQ, heads, DV)
    grad_weights = jnp.einsum(
        "nqhc,nkhc->nhqk", grad_mixed, values, preferred_element_type=F32
    )
    grad_scores = (
        weights * (grad_weights - jnp.sum(weights * grad_weights, axis=-1, keepdims=True))
    ).astype(BF)
    grad_values = jnp.einsum(
        "nhqk,nqhc->nkhc", weights.astype(BF), grad_mixed, preferred_element_type=F32
    )
    grad_queries = (
        jnp.einsum("nhqk,nkhc->nqhc", grad_scores, keys, preferred_element_type=F32) * scale
    )
    grad_keys = (
        jnp.einsum("nhqk,nqhc->nkhc", grad_scores, queries, preferred_element_type=F32) * scale
    )
    grad_query = (
        jnp.concatenate(
            [
                grad_queries[..., :DN],
                unrotate(grad_queries[..., DN:], cosine[:, None, :], sine[:, None, :]),
            ],
            axis=-1,
        )
        .astype(BF)
        .reshape(count, heads * (DN + DR))
    )
    step_query = matmul_cols(normed, grad_query)
    query_part = matmul_rows(grad_query, full_query)
    rope_part = unrotate(jnp.sum(grad_keys[..., DN:], axis=2), cosine, sine).reshape(count, DR)
    grad_expanded = (
        jnp.concatenate([grad_keys[..., :DN], grad_values], axis=-1)
        .astype(BF)
        .reshape(count, heads * (DN + DV))
    )
    step_expand = matmul_cols(latent_normed, grad_expanded)
    expand_back = (
        step_expand.astype(BF)
        .reshape(groups, er, fold, cut)
        .transpose(0, 2, 1, 3)
        .reshape(groups * rows_dev, cut)
    )
    qe_sum = scatter_rows(
        jnp.concatenate([step_query.astype(BF), expand_back], axis=1).reshape(groups, rows_dev, -1)
    )
    latent_part = matmul_rows(grad_expanded, full_expand)
    lat_part = jnp.concatenate([latent_part, rope_part], axis=1).astype(BF)
    lat_part = add(lat_part, to_core(lat_part))
    latent_sum = lat_part.astype(F32) + to_y(lat_part).astype(F32)
    grad_lnormed = latent_sum[:, :KV_RANK]
    step_gain_latent = jnp.sum(grad_lnormed * latent_hat, axis=0)
    grad_compressed = norm_back(grad_lnormed * gain_kv, latent_hat, latent_scale)
    grad_lat = jnp.concatenate([grad_compressed, latent_sum[:, KV_RANK:]], axis=-1).astype(BF)
    query_sum = scatter_cols(query_part.astype(BF))
    latent_slice = lax.dynamic_slice_in_dim(full_latent, place_t * width, width, 0)
    grad_normed = (
        query_sum[0].astype(F32) + query_sum[1].astype(F32) + matmul_rows(grad_lat, latent_slice)
    )
    first_hat_slice = lax.dynamic_slice_in_dim(first_hat, place_t * width, width, 1)
    gain_first_slice = lax.dynamic_slice_in_dim(gain_first, place_t * width, width, 0)
    grad_hat = grad_normed * gain_first_slice
    row_dot = small_sum(jnp.sum(grad_hat * first_hat_slice, axis=1).reshape(-1, 128)) / D
    grad_middle_slice = lax.dynamic_slice_in_dim(grad_middle, place_t * width, width, 1)
    input_grad = grad_middle_slice + first_scale * (
        grad_hat - first_hat_slice * row_dot.reshape(-1, 1)
    )
    step_gain_one = jnp.sum(grad_normed * first_hat_slice, axis=0)

    normed_part = lax.dynamic_index_in_dim(
        normed.reshape(count, groups, tensors, quarter), place_t, 2, keepdims=False
    ).reshape(count, groups * quarter)
    step_latent = matmul_cols(normed_part, grad_lat).reshape(groups, quarter, lc)
    one_full = lax.dynamic_update_slice_in_dim(
        jnp.zeros((D,), F32), step_gain_one, place_t * width, 0
    )
    once = jnp.where(place_t == 0, 1.0, 0.0)
    gain_rows = jnp.concatenate(
        [
            one_full.reshape(groups, rows_dev),
            (step_gain_two * once).reshape(groups, rows_dev),
            (step_gain_latent * once).reshape(groups, kv_dev),
        ],
        axis=1,
    )
    lat_sum = add(
        *scatter_rows(jnp.concatenate([step_latent, gain_rows[:, None]], axis=1).astype(BF))
    )
    lat_pieces = pieces_of(lat_sum)
    gain_sum = sum(piece[quarter].astype(F32) for piece in lat_pieces)
    grad_latent = join([piece[:quarter] for piece in lat_pieces], 0).astype(F32)
    qe = qe_sum[0].astype(F32) + qe_sum[1].astype(F32)
    grad_expand = jnp.concatenate(
        [qe[i * er : (i + 1) * er, qc:] for i in range(fold)], axis=1
    )
    return (
        block_out,
        input_grad,
        gain_sum[:rows_dev],
        qe[:, :qc],
        grad_latent,
        gain_sum[2 * rows_dev :],
        grad_expand,
        output_sum[0].astype(F32) + output_sum[1].astype(F32),
        gain_sum[rows_dev : 2 * rows_dev],
        shared_step[0],
        shared_step[1],
        shared_step[2],
        total_gate,
        total_up,
        total_down,
    )


def solution(mesh):
    body = local if mesh.shape["expert"] == 8 and mesh.shape["tensor"] == 4 else local_wide
    both = P("expert", "tensor")
    cols = P("expert", None, "tensor")
    rows = P("expert", "tensor", None)
    one = P("expert")
    flat = P("expert", None)
    return jax.shard_map(
        body,
        mesh=mesh,
        in_specs=(
            both, both, one, both, flat, one, both, both, one, both, both, both,
            cols, cols, rows, flat, flat,
        ),
        out_specs=(
            both, both, one, both, flat, one, both, both, one, both, both, both,
            cols, cols, rows,
        ),
        check_vma=False,
    )
```
